256 devices in a mesh: gx: 16 (over x, y_lo, core), gy: 16 (over y_hi, z).
Axes of the slice: x: 4, y: 4 (y_hi: 2, y_lo: 2; y = y_hi * 2 + y_lo), z: 8, core: 2. Of those that a mesh axis runs over, the one named last changes fastest.
Arguments:
- spectrum: float32 [384, 640, 1080], P('gx', 'gy'), may hold values from 0.05 to 1
- adjoint_in: float32 [384, 640, 1080], P('gx', 'gy'), may hold values from 0 to 2
- current_x: float32 [384, 640], P('gx', 'gy'), may hold values from -0.08 to 0.08
- current_y: float32 [384, 640], P('gx', 'gy'), may hold values from -0.08 to 0.08
- wind_x: float32 [384, 640], P('gx', 'gy'), may hold values from -4 to 4
- wind_y: float32 [384, 640], P('gx', 'gy'), may hold values from -4 to 4
- land_mask: int32 [384, 640], P('gx', 'gy'), may hold values from 0 to 1, as said below
- ice_mask: int32 [384, 640], P('gx', 'gy'), may hold values from 0 to 1, as said below
- group_speed: float32 [30], replicated, may hold values from 0.1 to 0.4
- growth_rate: float32 [30], replicated, may hold values from 0.1 to 1
- dissipation: float32 [30], replicated, may hold values from 0.3 to 3
Outputs:
- adjoint_spectrum: float32 [384, 640, 1080], P('gx', 'gy')
The draws below stay inside these ranges and needn't reach their ends.
Inputs may be any that keep to these rules, and one draw needn't show every extreme that they name: `land_mask`: 1 marks land, 0 sea. `ice_mask`: 1 marks sea ice, 0 open water.
All inputs are finite; a program needn't handle non-finite values.
Results may differ from the reference program's by a relative error of at most 0.0001.
Values sent between devices are 32-bit elements; how exact they have to be, the bound alone decides.
A program may use at most 128 MiB of HBM per device.

```python
import math
import jax
import jax.numpy as jnp
from jax import lax

DIRS = 36
FREQS = 30
BINS = 1080
CX = 24
CY = 40
NX = 384
NY = 640


def draw_land_mask(key, part):
    islands = max(2, NX * NY // (8 * CX * CY))
    centre_x = jax.random.randint(jax.random.fold_in(key, 1), (islands,), 0, NX)
    centre_y = jax.random.randint(jax.random.fold_in(key, 2), (islands,), 0, NY)
    radius = jax.random.randint(jax.random.fold_in(key, 3), (islands,), max(1, min(CX, CY) // 2), max(CX, CY) + 1)
    row_index = jnp.arange(NX, dtype=jnp.int32)
    col_index = jnp.arange(NY, dtype=jnp.int32)
    gap_x = jnp.abs(row_index[None, :] - centre_x[:, None])
    gap_x = jnp.minimum(gap_x, NX - gap_x)
    gap_y = jnp.abs(col_index[None, :] - centre_y[:, None])
    inside = gap_x[:, :, None] * gap_x[:, :, None] + gap_y[:, None, :] * gap_y[:, None, :] < (radius * radius)[:, None, None]
    return jnp.any(inside, axis=0).astype(jnp.int32)


def draw_ice_mask(key, part):
    ice_reach = max(2, NY // 8)
    south_edge = jax.random.randint(jax.random.fold_in(key, 11), (NX, 1), 0, ice_reach)
    north_edge = jax.random.randint(jax.random.fold_in(key, 12), (NX, 1), 0, ice_reach)
    col_index = jnp.arange(NY, dtype=jnp.int32)[None, :]
    frozen = (col_index < south_edge) | (col_index >= NY - north_edge)
    return frozen.astype(jnp.int32)


def shard_levels(own_key, extent, split, smallest, largest):
    gain = 1.0
    for axis_at, blocks in split:
        heights = jax.random.uniform(jax.random.fold_in(jax.random.fold_in(own_key, 6), axis_at), (blocks,), jnp.float32, smallest / len(split), largest / len(split))
        gain = gain * jnp.repeat(jnp.exp(heights), extent[axis_at] // blocks).reshape((-1,) + (1,) * (len(extent) - 1 - axis_at))
    return gain


def bell_draw(own_key, shape, scale, most, split=(), held_as=jnp.bfloat16):
    loudness = shard_levels(own_key, shape, split, -0.22, 0.18) if split else 1.0
    entries = jax.random.normal(own_key, shape, jnp.float32) * scale * loudness
    return jnp.minimum(jnp.maximum(entries, -most), most).astype(held_as)


def setup_inputs(seed: int = 0) -> dict:
    key_of = jax.random.split(jax.random.key(seed), 12)
    return {
        "spectrum": jnp.clip(jnp.exp(math.log(1.0) - 2.9957323 * jax.random.uniform(key_of[0], (NX, NY, BINS), jnp.float32) ** shard_levels(key_of[0], (NX, NY, BINS), ((0, 16), (1, 16)), -0.2, 0.2)), 0.05, 1.0),
        "adjoint_in": jnp.clip(2.0 * jax.random.uniform(key_of[1], (NX, NY, BINS), jnp.float32) ** shard_levels(key_of[1], (NX, NY, BINS), ((0, 16), (1, 16)), -0.2, 0.2), 0.0, 2.0),
        "current_x": jnp.clip(jax.random.uniform(key_of[2], (NX, NY), jnp.float32, -0.08, 0.08) * shard_levels(key_of[2], (NX, NY), ((0, 16), (1, 16)), -0.4, 0.0), -0.08, 0.08),
        "current_y": jnp.clip(jax.random.uniform(key_of[3], (NX, NY), jnp.float32, -0.08, 0.08) * shard_levels(key_of[3], (NX, NY), ((0, 16), (1, 16)), -0.4, 0.0), -0.08, 0.08),
        "wind_x": bell_draw(key_of[4], (NX, NY), 1.0, 4.0, ((0, 16), (1, 16)), jnp.float32),
        "wind_y": bell_draw(key_of[5], (NX, NY), 1.0, 4.0, ((0, 16), (1, 16)), jnp.float32),
        "land_mask": draw_land_mask(jax.random.fold_in(key_of[11], 71), 0),
        "ice_mask": draw_ice_mask(jax.random.fold_in(key_of[11], 71), 0),
        "group_speed": jnp.clip(jnp.exp(jax.random.uniform(key_of[8], (FREQS,), jnp.float32, math.log(0.1), math.log(0.4))), 0.1, 0.4),
        "growth_rate": jnp.clip(jnp.exp(jax.random.uniform(key_of[9], (FREQS,), jnp.float32, math.log(0.1), math.log(1.0))), 0.1, 1.0),
        "dissipation": jnp.clip(jnp.exp(jax.random.uniform(key_of[10], (FREQS,), jnp.float32, math.log(0.3), math.log(3.0))), 0.3, 3.0),
    }


def shift_north(values):
    return jnp.concatenate([values[:, 1:], jnp.zeros_like(values[:, :1])], axis=1)


def shift_south(values):
    return jnp.concatenate([jnp.zeros_like(values[:, :1]), values[:, :-1]], axis=1)


def reference(spectrum, adjoint_in, current_x, current_y, wind_x, wind_y, land_mask, ice_mask, group_speed, growth_rate, dissipation):
    sea_mask = (1 - land_mask).astype(jnp.float32)
    ice_free = (1 - ice_mask).astype(jnp.float32)
    angles = (2.0 * math.pi / DIRS) * (jnp.arange(DIRS, dtype=jnp.float32) + 0.5)
    open_lon = sea_mask * jnp.roll(sea_mask, -1, axis=0)
    drift_lon = 0.5 * (current_x + jnp.roll(current_x, -1, axis=0))
    open_lat = sea_mask * shift_north(sea_mask)
    drift_lat = 0.5 * (current_y + shift_north(current_y))

    def forward_block(direction):
        offset = (direction * FREQS).astype(jnp.int32)
        block_field = lax.dynamic_slice_in_dim(spectrum, offset, FREQS, 2)
        cosine = jnp.cos(angles[direction])
        sine_val = jnp.sin(angles[direction])
        lon_courant = open_lon[..., None] * (group_speed * cosine + drift_lon[..., None])
        lat_courant = open_lat[..., None] * (group_speed * sine_val + drift_lat[..., None])
        lon_plus = jnp.maximum(lon_courant, 0.0)
        lon_minus = jnp.minimum(lon_courant, 0.0)
        lat_plus = jnp.maximum(lat_courant, 0.0)
        lat_minus = jnp.minimum(lat_courant, 0.0)
        lon_flux = lon_plus * block_field + lon_minus * jnp.roll(block_field, -1, axis=0)
        lat_flux = lat_plus * block_field + lat_minus * shift_north(block_field)
        advected = block_field - (lon_flux - jnp.roll(lon_flux, 1, axis=0)) - (lat_flux - shift_south(lat_flux))
        return advected, lon_plus, lon_minus, lat_plus, lat_minus, offset, cosine, sine_val

    def add_energy(direction, running):
        advected = forward_block(direction)[0]
        return running + jnp.sum(advected, axis=2)

    energy = lax.fori_loop(0, DIRS, add_energy, jnp.zeros((NX, NY), jnp.float32)) / BINS

    def weigh_block(direction):
        advected, lon_plus, lon_minus, lat_plus, lat_minus, offset, cosine, sine_val = forward_block(direction)
        incoming = lax.dynamic_slice_in_dim(adjoint_in, offset, FREQS, 2)
        project = wind_x[..., None] * cosine + wind_y[..., None] * sine_val
        gained = 1.0 + growth_rate * jnp.maximum(project, 0.0) * ice_free[..., None]
        damped = 1.0 + dissipation * energy[..., None] * advected
        weighted = incoming * gained / (damped * damped)
        return advected, weighted, lon_plus, lon_minus, lat_plus, lat_minus, offset

    def add_coupling(direction, running):
        parts = weigh_block(direction)
        advected, weighted = parts[0], parts[1]
        return running + jnp.sum(weighted * dissipation * advected * advected, axis=2)

    coupling = lax.fori_loop(0, DIRS, add_coupling, jnp.zeros((NX, NY), jnp.float32))

    def adjoint_block(direction, output):
        advected, weighted, lon_plus, lon_minus, lat_plus, lat_minus, offset = weigh_block(direction)
        sensitivity = sea_mask[..., None] * (weighted - coupling[..., None] / BINS)
        lon_step = jnp.roll(sensitivity, -1, axis=0) - sensitivity
        lat_step = shift_north(sensitivity) - sensitivity
        result = sensitivity + lon_plus * lon_step + jnp.roll(lon_minus * lon_step, 1, axis=0)
        result = result + lat_plus * lat_step + shift_south(lat_minus * lat_step)
        return lax.dynamic_update_slice_in_dim(output, result, offset, 2)

    return lax.fori_loop(0, DIRS, adjoint_block, jnp.zeros((NX, NY, BINS), jnp.float32))
```

```python
import math

import jax
import jax.numpy as jnp
import numpy as np
from jax import lax
from jax.experimental import pallas as pl
from jax.experimental.pallas import tpu as pltpu
from jax.sharding import PartitionSpec as P

DIRS = 36
LANES = 128
PAD = 8
MESH = pl.DeviceIdType.MESH


def kernel(
    spec_hbm,
    adj_hbm,
    cx_hbm,
    cy_hbm,
    wx_hbm,
    wy_hbm,
    land_hbm,
    ice_hbm,
    tab_hbm,
    out,
    sp_main,
    sp_tail,
    ss_main,
    ss_tail,
    inc,
    adv,
    oxs,
    pxs,
    oys,
    pys,
    wxs,
    wys,
    seas,
    tab_in,
    tab,
    stat_f,
    stat_i,
    nb_f,
    nb_i,
    ext,
    load_sem,
    send_sem,
    recv_sem,
):
    rows, cols, bins = spec_hbm.shape
    mains = bins // LANES
    tail = bins - mains * LANES
    tiles = cols // 8
    pieces = mains + 1
    gx = lax.axis_index("gx")
    gy = lax.axis_index("gy")
    nx = lax.axis_size("gx")
    ny = lax.axis_size("gy")
    east = lax.rem(gx + 1, nx)
    west = lax.rem(gx + nx - 1, nx)
    has_north = gy < ny - 1
    has_south = gy > 0
    body = pl.ds(PAD, cols)

    def local(src, dst, k):
        return pltpu.make_async_copy(src, dst, load_sem.at[k])

    def loads_of(low, count, base):
        copies = []
        for t in range(pieces):
            src_lanes = pl.ds(t * LANES, LANES if t < mains else tail)
            src = spec_hbm.at[pl.ds(low, count), :, src_lanes]
            if t < mains:
                dst = sp_main.at[pl.ds(low + 1, count), t, body, :]
            else:
                dst = sp_tail.at[pl.ds(low + 1, count), body, :]
            copies.append(local(src, dst, base + t))
        return copies

    first_row = loads_of(0, 1, 0)
    last_row = loads_of(rows - 1, 1, pieces)
    bulk = loads_of(1, rows - 2, 2 * pieces)
    base = 3 * pieces
    small = [
        local(land_hbm, stat_i.at[0], base),
        local(cx_hbm, stat_f.at[0], base + 1),
        local(cy_hbm, stat_f.at[1], base + 2),
        local(wx_hbm, stat_f.at[2], base + 3),
        local(wy_hbm, stat_f.at[3], base + 4),
        local(ice_hbm, stat_i.at[1], base + 5),
        local(tab_hbm, tab_in, base + 6),
    ]
    inc_load = local(adj_hbm, inc, base + 7)
    for copy in small + last_row + first_row + bulk + [inc_load]:
        copy.start()

    barrier = pltpu.get_barrier_semaphore()
    for target in (east, west):
        pl.semaphore_signal(barrier, inc=1, device_id={"gx": target}, device_id_type=MESH)

    @pl.when(has_north)
    def _():
        pl.semaphore_signal(barrier, inc=1, device_id={"gy": gy + 1}, device_id_type=MESH)

    @pl.when(has_south)
    def _():
        pl.semaphore_signal(barrier, inc=1, device_id={"gy": gy - 1}, device_id_type=MESH)

    def zero_line(line):
        def step(r, carry):
            for main, last in ((sp_main, sp_tail), (ss_main, ss_tail)):
                for t in range(mains):
                    main[r, t, pl.ds(line, 1), :] = jnp.zeros((1, LANES), jnp.float32)
                last[r, pl.ds(line, 1), :] = jnp.zeros((1, tail), jnp.float32)
            return carry

        lax.fori_loop(1, rows + 1, step, 0)

    @pl.when(gy == 0)
    def _():
        zero_line(PAD - 1)

    @pl.when(gy == ny - 1)
    def _():
        zero_line(PAD + cols)

    peers = 2 + lax.div(gy + ny - 1, ny) + lax.div(2 * ny - 2 - gy, ny)
    pl.semaphore_wait(barrier, peers)

    def remote(src, dst, k, device):
        return pltpu.make_async_remote_copy(
            src_ref=src,
            dst_ref=dst,
            send_sem=send_sem.at[k],
            recv_sem=recv_sem.at[k],
            device_id=device,
            device_id_type=MESH,
        )

    to_east, to_west = {"gx": east}, {"gx": west}
    to_north, to_south = {"gy": gy + 1}, {"gy": gy - 1}

    def edge(main, last, k, side):
        inner = pl.ds(1, rows)
        if side == "east":
            src, dst = (rows, body), (0, body)
            device = to_east
        elif side == "west":
            src, dst = (1, body), (rows + 1, body)
            device = to_west
        elif side == "north":
            src = (inner, pl.ds(PAD + cols - 1, 1))
            dst = (inner, pl.ds(PAD - 1, 1))
            device = to_north
        else:
            src = (inner, pl.ds(PAD, 1))
            dst = (inner, pl.ds(PAD + cols, 1))
            device = to_south
        return [
            remote(main.at[src[0], :, src[1], :], main.at[dst[0], :, dst[1], :], k, device),
            remote(last.at[src[0], src[1], :], last.at[dst[0], dst[1], :], k + 1, device),
        ]

    sides = ("east", "west", "north", "south")
    stat_copies = {}
    for s, (side, device, field) in enumerate(
        (("east", to_east, 0), ("west", to_west, 0), ("north", to_north, 1), ("south", to_south, 1))
    ):
        stat_copies[side] = [
            remote(stat_i.at[0], nb_i.at[s], 16 + 2 * s, device),
            remote(stat_f.at[field], nb_f.at[s], 17 + 2 * s, device),
        ]
    one = {side: edge(sp_main, sp_tail, 2 * s, side) for s, side in enumerate(sides)}
    two = {side: edge(ss_main, ss_tail, 8 + 2 * s, side) for s, side in enumerate(sides)}

    sends_ok = {"east": None, "west": None, "north": has_north, "south": has_south}
    recvs_ok = {"east": None, "west": None, "north": has_south, "south": has_north}

    def guarded(condition, run):
        if condition is None:
            run()
        else:
            pl.when(condition)(run)

    def start(group, side):
        guarded(sends_ok[side], lambda: [copy.start() for copy in group[side]] and None)

    def wait_recv(group, side):
        guarded(recvs_ok[side], lambda: [copy.wait_recv() for copy in group[side]] and None)

    def wait_send(group, side):
        guarded(sends_ok[side], lambda: [copy.wait_send() for copy in group[side]] and None)

    for copy in small[:3]:
        copy.wait()
    for side in sides:
        start(stat_copies, side)
    for copy in last_row:
        copy.wait()
    start(one, "east")
    for copy in first_row:
        copy.wait()
    start(one, "west")
    for copy in bulk:
        copy.wait()
    start(one, "north")
    start(one, "south")

    for copy in small[3:]:
        copy.wait()
    for k in range(5):
        for t in range(pieces):
            width = LANES if t < mains else tail
            line = tab_in[pl.ds(k, 1), pl.ds(t * LANES, width)]
            tab[k * pieces + t, :, pl.ds(0, width)] = jnp.broadcast_to(line, (8, width))

    for side in sides:
        wait_recv(stat_copies, side)

    lane = lax.broadcasted_iota(jnp.int32, (32, LANES), 1)
    row = lax.broadcasted_iota(jnp.int32, (32, LANES), 0)

    def widened(values):
        ext[...] = jnp.zeros((32, LANES), jnp.float32)
        ext[pl.ds(0, rows), pl.ds(0, cols)] = values
        return ext[...]

    def sea_of(mask):
        return (1 - mask).astype(jnp.float32)

    def around_lon(mine, from_east, from_west):
        up = pltpu.roll(widened(from_east), rows, 0)
        down = pltpu.roll(widened(from_west), 8, 0)
        return jnp.where(row == rows, up, jnp.where(row == 31, down, mine))

    def around_lat(mine, from_north, from_south):
        up = pltpu.roll(widened(from_north), cols, 1)
        down = pltpu.roll(widened(from_south), LANES - cols, 1)
        up = jnp.where(has_north, up, 0.0)
        down = jnp.where(has_south, down, 0.0)
        return jnp.where(lane == cols, up, jnp.where(lane == LANES - 1, down, mine))

    sea = widened(sea_of(stat_i[0]))
    ice_free = widened(sea_of(stat_i[1]))
    sea_lon = around_lon(sea, sea_of(nb_i[1]), sea_of(nb_i[0]))
    sea_lat = around_lat(sea, sea_of(nb_i[3]), sea_of(nb_i[2]))
    drift_lon = around_lon(widened(stat_f[0]), nb_f[1], nb_f[0])
    drift_lat = around_lat(widened(stat_f[1]), nb_f[3], nb_f[2])
    open_lon = sea_lon * pltpu.roll(sea_lon, 31, 0)
    push_lon = open_lon * (0.5 * (drift_lon + pltpu.roll(drift_lon, 31, 0)))
    open_lat = sea_lat * pltpu.roll(sea_lat, LANES - 1, 1)
    push_lat = open_lat * (0.5 * (drift_lat + pltpu.roll(drift_lat, LANES - 1, 1)))
    wet = ice_free * sea
    wind_x = widened(stat_f[2]) * wet
    wind_y = widened(stat_f[3]) * wet

    def spread(field, dst, lat_faces=False, lon_faces=False):
        turned = jnp.transpose(field)
        if lon_faces:
            order = [31] + list(range(rows))
        else:
            order = list(range(rows))
        for at, r in enumerate(order):
            column = turned[:cols, r : r + 1]
            if lat_faces:
                dst[at, pl.ds(PAD, cols), :] = jnp.broadcast_to(column, (cols, LANES))
                first = turned[LANES - 1 :, r : r + 1]
                dst[at, pl.ds(PAD - 1, 1), :] = jnp.broadcast_to(first, (1, LANES))
            else:
                dst[at, :, :] = jnp.broadcast_to(column, (cols, LANES))

    spread(open_lon, oxs, lon_faces=True)
    spread(push_lon, pxs, lon_faces=True)
    spread(open_lat, oys, lat_faces=True)
    spread(push_lat, pys, lat_faces=True)
    spread(wind_x, wxs)
    spread(wind_y, wys)
    spread(sea, seas)

    def width_of(t):
        return LANES if t < mains else tail

    def at(main, last, r, t, line):
        if t < mains:
            return main[r, t, pl.ds(line, 8), :]
        return last[r, pl.ds(line, 8), :]

    def put(main, last, r, t, line, value):
        if t < mains:
            main[r, t, pl.ds(line, 8), :] = value
        else:
            last[r, pl.ds(line, 8), :] = value

    def table(k, t):
        return tab[k * pieces + t, :, pl.ds(0, width_of(t))]

    def faces(i, jt, t):
        cut = (slice(None), slice(0, width_of(t)))
        line = PAD + 8 * jt
        cos_speed, sin_speed = table(0, t), table(1, t)
        spot = pl.ds(8 * jt, 8)
        a_e = oxs[i + 1, spot, :][cut] * cos_speed + pxs[i + 1, spot, :][cut]
        a_w = oxs[i, spot, :][cut] * cos_speed + pxs[i, spot, :][cut]
        a_n = oys[i, pl.ds(line, 8), :][cut] * sin_speed + pys[i, pl.ds(line, 8), :][cut]
        a_s = oys[i, pl.ds(line - 1, 8), :][cut] * sin_speed + pys[i, pl.ds(line - 1, 8), :][cut]
        return a_e, a_w, a_n, a_s

    def around(main, last, i, jt, t):
        line = PAD + 8 * jt
        return (
            at(main, last, i + 1, t, line),
            at(main, last, i + 2, t, line),
            at(main, last, i, t, line),
            at(main, last, i + 1, t, line + 1),
            at(main, last, i + 1, t, line - 1),
        )

    def lane_sum(parts):
        whole = parts[0]
        for part in parts[1:mains]:
            whole = whole + part
        return jnp.sum(whole, axis=1, keepdims=True) + jnp.sum(parts[mains], axis=1, keepdims=True)

    scale = 1.0 / bins

    def source(cells):
        energies = []
        for u, (i, jt) in enumerate(cells):
            parts = []
            for t in range(pieces):
                a_e, a_w, a_n, a_s = faces(i, jt, t)
                here, e, w, n, s = around(sp_main, sp_tail, i, jt, t)
                lon = a_e * jnp.where(a_e > 0.0, here, e) - a_w * jnp.where(a_w > 0.0, w, here)
                lat = a_n * jnp.where(a_n > 0.0, here, n) - a_s * jnp.where(a_s > 0.0, s, here)
                moved = here - lon - lat
                adv[u, t, :, pl.ds(0, width_of(t))] = moved
                parts.append(moved)
            energies.append(lane_sum(parts) * scale)
        pulls = []
        for u, (i, jt) in enumerate(cells):
            parts = []
            spot = pl.ds(8 * jt, 8)
            energy = jnp.broadcast_to(energies[u], (8, LANES))
            for t in range(pieces):
                width = width_of(t)
                cut = (slice(None), slice(0, width))
                moved = adv[u, t, :, pl.ds(0, width)]
                blow = wxs[i, spot, :][cut] * table(2, t) + wys[i, spot, :][cut] * table(3, t)
                gain = jnp.maximum(blow, 0.0) + seas[i, spot, :][cut]
                loss = table(4, t) * moved
                damp = 1.0 + energy[cut] * loss
                square = damp * damp
                inverse = pl.reciprocal(square, approx=True)
                inverse = inverse * (2.0 - square * inverse)
                weighted = inc[i, spot, pl.ds(t * LANES, width)] * gain * inverse
                put(ss_main, ss_tail, i + 1, t, PAD + 8 * jt, weighted)
                parts.append(weighted * loss * moved)
            pulls.append(lane_sum(parts) * scale)
        for u, (i, jt) in enumerate(cells):
            pull = jnp.broadcast_to(pulls[u], (8, LANES))
            line = PAD + 8 * jt
            for t in range(pieces):
                value = at(ss_main, ss_tail, i + 1, t, line) - pull[:, : width_of(t)]
                put(ss_main, ss_tail, i + 1, t, line, value)

    def transport(cells):
        for i, jt in cells:
            for t in range(pieces):
                a_e, a_w, a_n, a_s = faces(i, jt, t)
                here, e, w, n, s = around(ss_main, ss_tail, i, jt, t)
                lon = jnp.maximum(a_e, 0.0) * (e - here) + jnp.minimum(a_w, 0.0) * (here - w)
                lat = jnp.maximum(a_n, 0.0) * (n - here) + jnp.minimum(a_s, 0.0) * (here - s)
                out[i, pl.ds(8 * jt, 8), pl.ds(t * LANES, width_of(t))] = here + lon + lat

    def looped(low, high, run):
        def step(i, carry):
            run(i)
            return carry

        lax.fori_loop(low, high, step, 0)

    inc_load.wait()
    middle = range(1, tiles - 1)
    looped(1, rows - 1, lambda i: source([(i, jt) for jt in middle]))
    wait_recv(one, "west")
    wait_recv(one, "east")
    wait_recv(one, "north")
    wait_recv(one, "south")
    source([(rows - 1, jt) for jt in range(tiles)])
    start(two, "east")
    source([(0, jt) for jt in range(tiles)])
    start(two, "west")
    looped(1, rows - 1, lambda i: source([(i, 0), (i, tiles - 1)]))
    start(two, "north")
    start(two, "south")
    looped(1, rows - 1, lambda i: transport([(i, jt) for jt in middle]))
    for side in sides:
        wait_recv(two, side)
    looped(1, rows - 1, lambda i: transport([(i, 0), (i, tiles - 1)]))
    transport([(0, jt) for jt in range(tiles)])
    transport([(rows - 1, jt) for jt in range(tiles)])
    for group in (stat_copies, one, two):
        for side in sides:
            wait_send(group, side)


def body(
    spectrum,
    adjoint_in,
    current_x,
    current_y,
    wind_x,
    wind_y,
    land_mask,
    ice_mask,
    group_speed,
    growth_rate,
    dissipation,
):
    rows, cols, bins = spectrum.shape
    per_dir = bins // DIRS
    angles = np.float32(2.0 * math.pi / DIRS) * (np.arange(DIRS, dtype=np.float32) + np.float32(0.5))
    cosine = jnp.asarray(np.repeat(np.cos(angles), per_dir))
    sine = jnp.asarray(np.repeat(np.sin(angles), per_dir))
    speed = jnp.tile(group_speed, DIRS)
    growth = jnp.tile(growth_rate, DIRS)
    loss = jnp.tile(dissipation, DIRS)
    zero = jnp.zeros_like(loss)
    tables = jnp.stack(
        [speed * cosine, speed * sine, growth * cosine, growth * sine, loss, zero, zero, zero]
    )
    mains = bins // LANES
    tail = bins - mains * LANES
    tall = cols + 2 * PAD
    f32 = jnp.float32
    any_space = pl.BlockSpec(memory_space=pl.ANY)
    return pl.pallas_call(
        kernel,
        out_shape=jax.ShapeDtypeStruct((rows, cols, bins), f32),
        in_specs=[any_space] * 9,
        out_specs=pl.BlockSpec(memory_space=pltpu.VMEM),
        scratch_shapes=[
            pltpu.VMEM((rows + 2, mains, tall, LANES), f32),
            pltpu.VMEM((rows + 2, tall, tail), f32),
            pltpu.VMEM((rows + 2, mains, tall, LANES), f32),
            pltpu.VMEM((rows + 2, tall, tail), f32),
            pltpu.VMEM((rows, cols, bins), f32),
            pltpu.VMEM((cols // 8, mains + 1, 8, LANES), f32),
            pltpu.VMEM((rows + 1, cols, LANES), f32),
            pltpu.VMEM((rows + 1, cols, LANES), f32),
            pltpu.VMEM((rows, tall, LANES), f32),
            pltpu.VMEM((rows, tall, LANES), f32),
            pltpu.VMEM((rows, cols, LANES), f32),
            pltpu.VMEM((rows, cols, LANES), f32),
            pltpu.VMEM((rows, cols, LANES), f32),
            pltpu.VMEM((8, bins), f32),
            pltpu.VMEM((5 * (mains + 1), 8, LANES), f32),
            pltpu.VMEM((4, rows, cols), f32),
            pltpu.VMEM((2, rows, cols), jnp.int32),
            pltpu.VMEM((4, rows, cols), f32),
            pltpu.VMEM((4, rows, cols), jnp.int32),
            pltpu.VMEM((32, LANES), f32),
            pltpu.SemaphoreType.DMA((3 * (mains + 1) + 8,)),
            pltpu.SemaphoreType.DMA((24,)),
            pltpu.SemaphoreType.DMA((24,)),
        ],
        compiler_params=pltpu.CompilerParams(
            collective_id=0, has_side_effects=True, vmem_limit_bytes=56 * 1024 * 1024
        ),
    )(
        spectrum,
        adjoint_in,
        current_x,
        current_y,
        wind_x,
        wind_y,
        land_mask,
        ice_mask,
        tables,
    )


def solution(mesh):
    cells = P("gx", "gy", None)
    placed = (cells, cells) + (P("gx", "gy"),) * 6 + (P(),) * 3
    return jax.shard_map(body, mesh=mesh, in_specs=placed, out_specs=cells, check_vma=False)
```

```python
import math

import jax
import jax.numpy as jnp
import numpy as np
from jax import lax
from jax.experimental import pallas as pl
from jax.experimental.pallas import tpu as pltpu
from jax.sharding import PartitionSpec as P

DIRS = 36
LANES = 128
PAD = 8
MESH = pl.DeviceIdType.MESH


def kernel(
    spec_hbm,
    adj_hbm,
    cx_hbm,
    cy_hbm,
    wx_hbm,
    wy_hbm,
    land_hbm,
    ice_hbm,
    speed_hbm,
    growth_hbm,
    loss_hbm,
    wave_hbm,
    out,
    sp_main,
    sp_tail,
    ss_main,
    ss_tail,
    inc,
    adv,
    oxs,
    pxs,
    oys,
    pys,
    wxs,
    wys,
    seas,
    fx,
    part,
    level,
    par_in,
    wave,
    par,
    tab,
    stat_f,
    stat_i,
    nb_f,
    nb_i,
    ext,
    load_sem,
    send_sem,
    recv_sem,
):
    rows, cols, bins = spec_hbm.shape
    mains = bins // LANES
    tail = bins - mains * LANES
    tiles = cols // 8
    pieces = mains + 1
    gx = lax.axis_index("gx")
    gy = lax.axis_index("gy")
    nx = lax.axis_size("gx")
    ny = lax.axis_size("gy")
    east = lax.rem(gx + 1, nx)
    west = lax.rem(gx + nx - 1, nx)
    has_north = gy < ny - 1
    has_south = gy > 0
    body = pl.ds(PAD, cols)

    def local(src, dst, k):
        return pltpu.make_async_copy(src, dst, load_sem.at[k])

    def loads_of(low, count, base):
        copies = []
        for t in range(pieces):
            src_lanes = pl.ds(t * LANES, LANES if t < mains else tail)
            src = spec_hbm.at[pl.ds(low, count), :, src_lanes]
            if t < mains:
                dst = sp_main.at[pl.ds(low + 1, count), t, body, :]
            else:
                dst = sp_tail.at[pl.ds(low + 1, count), body, :]
            copies.append(local(src, dst, base + t))
        return copies

    first_row = loads_of(0, 1, 0)
    last_row = loads_of(rows - 1, 1, pieces)
    bulk = loads_of(1, rows - 2, 2 * pieces)
    base = 3 * pieces
    small = [
        local(land_hbm, stat_i.at[0], base),
        local(cx_hbm, stat_f.at[0], base + 1),
        local(cy_hbm, stat_f.at[1], base + 2),
        local(wx_hbm, stat_f.at[2], base + 3),
        local(wy_hbm, stat_f.at[3], base + 4),
        local(ice_hbm, stat_i.at[1], base + 5),
        local(speed_hbm, par_in.at[0], base + 6),
        local(growth_hbm, par_in.at[1], base + 7),
        local(loss_hbm, par_in.at[2], base + 8),
        local(wave_hbm, wave, base + 9),
    ]
    inc_load = local(adj_hbm, inc, base + 10)
    for copy in small + last_row + first_row + bulk + [inc_load]:
        copy.start()

    barrier = pltpu.get_barrier_semaphore()
    for target in (east, west):
        pl.semaphore_signal(barrier, inc=1, device_id={"gx": target}, device_id_type=MESH)

    @pl.when(has_north)
    def _():
        pl.semaphore_signal(barrier, inc=1, device_id={"gy": gy + 1}, device_id_type=MESH)

    @pl.when(has_south)
    def _():
        pl.semaphore_signal(barrier, inc=1, device_id={"gy": gy - 1}, device_id_type=MESH)

    def zero_line(line):
        def step(r, carry):
            for main, last in ((sp_main, sp_tail), (ss_main, ss_tail)):
                for t in range(mains):
                    main[r, t, pl.ds(line, 1), :] = jnp.zeros((1, LANES), jnp.float32)
                last[r, pl.ds(line, 1), :] = jnp.zeros((1, tail), jnp.float32)
            return carry

        lax.fori_loop(1, rows + 1, step, 0)

    @pl.when(gy == 0)
    def _():
        zero_line(PAD - 1)

    @pl.when(gy == ny - 1)
    def _():
        zero_line(PAD + cols)

    def remote(src, dst, k, device):
        return pltpu.make_async_remote_copy(
            src_ref=src,
            dst_ref=dst,
            send_sem=send_sem.at[k],
            recv_sem=recv_sem.at[k],
            device_id=device,
            device_id_type=MESH,
        )

    to_east, to_west = {"gx": east}, {"gx": west}
    to_north, to_south = {"gy": gy + 1}, {"gy": gy - 1}

    def edge(main, last, k, side):
        inner = pl.ds(1, rows)
        if side == "east":
            src, dst = (rows, body), (0, body)
            device = to_east
        elif side == "west":
            src, dst = (1, body), (rows + 1, body)
            device = to_west
        elif side == "north":
            src = (inner, pl.ds(PAD + cols - 1, 1))
            dst = (inner, pl.ds(PAD - 1, 1))
            device = to_north
        else:
            src = (inner, pl.ds(PAD, 1))
            dst = (inner, pl.ds(PAD + cols, 1))
            device = to_south
        return [
            remote(main.at[src[0], :, src[1], :], main.at[dst[0], :, dst[1], :], k, device),
            remote(last.at[src[0], src[1], :], last.at[dst[0], dst[1], :], k + 1, device),
        ]

    sides = ("east", "west", "north", "south")
    stat_copies = {}
    for s, (side, device, field) in enumerate(
        (("east", to_east, 0), ("west", to_west, 0), ("north", to_north, 1), ("south", to_south, 1))
    ):
        stat_copies[side] = [
            remote(stat_i.at[0], nb_i.at[s], 16 + 2 * s, device),
            remote(stat_f.at[field], nb_f.at[s], 17 + 2 * s, device),
        ]
    one = {side: edge(sp_main, sp_tail, 2 * s, side) for s, side in enumerate(sides)}
    two = {side: edge(ss_main, ss_tail, 8 + 2 * s, side) for s, side in enumerate(sides)}

    sends_ok = {"east": None, "west": None, "north": has_north, "south": has_south}
    recvs_ok = {"east": None, "west": None, "north": has_south, "south": has_north}

    def guarded(condition, run):
        if condition is None:
            run()
        else:
            pl.when(condition)(run)

    def start(group, side):
        guarded(sends_ok[side], lambda: [copy.start() for copy in group[side]] and None)

    def wait_recv(group, side):
        guarded(recvs_ok[side], lambda: [copy.wait_recv() for copy in group[side]] and None)

    def wait_send(group, side):
        guarded(sends_ok[side], lambda: [copy.wait_send() for copy in group[side]] and None)

    lane = lax.broadcasted_iota(jnp.int32, (32, LANES), 1)
    row = lax.broadcasted_iota(jnp.int32, (32, LANES), 0)

    def widened(values):
        ext[...] = jnp.zeros((32, LANES), jnp.float32)
        ext[pl.ds(0, rows), pl.ds(0, cols)] = values
        return ext[...]

    def sea_of(mask):
        return (1 - mask).astype(jnp.float32)

    def around_lon(mine, from_east, from_west):
        up = pltpu.roll(widened(from_east), rows, 0)
        down = pltpu.roll(widened(from_west), 8, 0)
        return jnp.where(row == rows, up, jnp.where(row == 31, down, mine))

    def around_lat(mine, from_north, from_south):
        up = pltpu.roll(widened(from_north), cols, 1)
        down = pltpu.roll(widened(from_south), LANES - cols, 1)
        up = jnp.where(has_north, up, 0.0)
        down = jnp.where(has_south, down, 0.0)
        return jnp.where(lane == cols, up, jnp.where(lane == LANES - 1, down, mine))

    def spread(field, places):
        turned = jnp.transpose(field)
        for dst, spot, column, r in places:
            count = column.stop - column.start
            dst[spot] = jnp.broadcast_to(turned[column, r : r + 1], (count, LANES))

    inside = slice(0, cols)
    inside_at = pl.ds(PAD, cols)

    def lon_faces(sea_lon, drift_lon):
        opened = sea_lon * pltpu.roll(sea_lon, 31, 0)
        return opened, opened * (0.5 * (drift_lon + pltpu.roll(drift_lon, 31, 0)))

    def lat_faces(sea_lat, drift_lat):
        opened = sea_lat * pltpu.roll(sea_lat, LANES - 1, 1)
        return opened, opened * (0.5 * (drift_lat + pltpu.roll(drift_lat, LANES - 1, 1)))

    def prepare():
        for copy in small[3:]:
            copy.wait()
        par[...] = jnp.zeros((8, LANES), jnp.float32)
        freqs = speed_hbm.shape[1]
        for k in range(3):
            par[pl.ds(k, 1), pl.ds(0, freqs)] = par_in[k]
        per_freq = par[...]
        bin_lane = lax.broadcasted_iota(jnp.int32, (8, LANES), 1)
        for t in range(pieces):
            freq = lax.rem(bin_lane + t * LANES, freqs)
            picked = jnp.take_along_axis(per_freq, freq, axis=1)
            full = (8, LANES)
            speed = jnp.broadcast_to(picked[0:1], full)
            growth = jnp.broadcast_to(picked[1:2], full)
            cosine = jnp.broadcast_to(wave[pl.ds(0, 1), pl.ds(t * LANES, LANES)], full)
            sine = jnp.broadcast_to(wave[pl.ds(1, 1), pl.ds(t * LANES, LANES)], full)
            tab[t] = speed * cosine
            tab[pieces + t] = speed * sine
            tab[2 * pieces + t] = growth * cosine
            tab[3 * pieces + t] = growth * sine
            tab[4 * pieces + t] = jnp.broadcast_to(picked[2:3], full)
        sea = widened(sea_of(stat_i[0]))
        wet = widened(sea_of(stat_i[1])) * sea
        every = range(rows)
        spread(sea, [(seas, r, inside, r) for r in every])
        spread(widened(stat_f[2]) * wet, [(wxs, r, inside, r) for r in every])
        spread(widened(stat_f[3]) * wet, [(wys, r, inside, r) for r in every])
        for field, dst in zip(lon_faces(sea, widened(stat_f[0])), (oxs, pxs)):
            spread(field, [(dst, r + 1, inside, r) for r in range(rows - 1)])
        for field, dst in zip(lat_faces(sea, widened(stat_f[1])), (oys, pys)):
            spread(field, [(dst, (r, inside_at), inside, r) for r in every])

    def prepare_edges():
        sea = widened(sea_of(stat_i[0]))
        sea_lon = around_lon(sea, sea_of(nb_i[1]), sea_of(nb_i[0]))
        sea_lat = around_lat(sea, sea_of(nb_i[3]), sea_of(nb_i[2]))
        drift_lon = around_lon(widened(stat_f[0]), nb_f[1], nb_f[0])
        drift_lat = around_lat(widened(stat_f[1]), nb_f[3], nb_f[2])
        for field, dst in zip(lon_faces(sea_lon, drift_lon), (oxs, pxs)):
            spread(field, [(dst, 0, inside, 31), (dst, rows, inside, rows - 1)])
        last, before = slice(cols - 1, cols), slice(LANES - 1, LANES)
        for field, dst in zip(lat_faces(sea_lat, drift_lat), (oys, pys)):
            spread(
                field,
                [(dst, (r, pl.ds(PAD - 1, 1)), before, r) for r in range(rows)]
                + [(dst, (r, pl.ds(PAD + cols - 1, 1)), last, r) for r in range(rows)],
            )

    def width_of(t):
        return LANES if t < mains else tail

    def at(main, last, r, t, line):
        if t < mains:
            return main[r, t, pl.ds(line, 8), :]
        return last[r, pl.ds(line, 8), :]

    def put(main, last, r, t, line, value):
        if t < mains:
            main[r, t, pl.ds(line, 8), :] = value
        else:
            last[r, pl.ds(line, 8), :] = value

    def table(k, t):
        return tab[k * pieces + t, :, pl.ds(0, width_of(t))]

    def faces(i, jt, t):
        cut = (slice(None), slice(0, width_of(t)))
        line = PAD + 8 * jt
        cos_speed, sin_speed = table(0, t), table(1, t)
        spot = pl.ds(8 * jt, 8)
        a_e = oxs[i + 1, spot, :][cut] * cos_speed + pxs[i + 1, spot, :][cut]
        a_w = oxs[i, spot, :][cut] * cos_speed + pxs[i, spot, :][cut]
        a_n = oys[i, pl.ds(line, 8), :][cut] * sin_speed + pys[i, pl.ds(line, 8), :][cut]
        a_s = oys[i, pl.ds(line - 1, 8), :][cut] * sin_speed + pys[i, pl.ds(line - 1, 8), :][cut]
        return a_e, a_w, a_n, a_s

    def around(main, last, i, jt, t):
        line = PAD + 8 * jt
        return (
            at(main, last, i + 1, t, line),
            at(main, last, i + 2, t, line),
            at(main, last, i, t, line),
            at(main, last, i + 1, t, line + 1),
            at(main, last, i + 1, t, line - 1),
        )

    scale = 1.0 / bins

    def lon_flux(i, jt, t):
        cut = (slice(None), slice(0, width_of(t)))
        spot = pl.ds(8 * jt, 8)
        line = PAD + 8 * jt
        pace = oxs[i + 1, spot, :][cut] * table(0, t) + pxs[i + 1, spot, :][cut]
        here, e = at(sp_main, sp_tail, i + 1, t, line), at(sp_main, sp_tail, i + 2, t, line)
        return pace * jnp.where(pace > 0.0, here, e)

    def tally(i, jt, parts):
        whole = parts[0]
        for more in parts[1:mains]:
            whole = whole + more
        part[i, jt] = whole
        part[i, jt, :, pl.ds(0, tail)] = whole[:, :tail] + parts[mains]

    def prime(i, jts):
        for jt in jts:
            for t in range(pieces):
                fx[jt, t, :, pl.ds(0, width_of(t))] = lon_flux(i - 1, jt, t)

    def advect(i, jts):
        for jt in jts:
            parts = []
            spot = pl.ds(PAD + 8 * jt, 8)
            under = pl.ds(PAD + 8 * jt - 1, 8)
            for t in range(pieces):
                width = width_of(t)
                cut = (slice(None), slice(0, width))
                sin_speed = table(1, t)
                a_n = oys[i, spot, :][cut] * sin_speed + pys[i, spot, :][cut]
                a_s = oys[i, under, :][cut] * sin_speed + pys[i, under, :][cut]
                line = PAD + 8 * jt
                here = at(sp_main, sp_tail, i + 1, t, line)
                n = at(sp_main, sp_tail, i + 1, t, line + 1)
                s = at(sp_main, sp_tail, i + 1, t, line - 1)
                f_w = fx[jt, t, :, pl.ds(0, width)]
                f_e = lon_flux(i, jt, t)
                fx[jt, t, :, pl.ds(0, width)] = f_e
                lat = a_n * jnp.where(a_n > 0.0, here, n) - a_s * jnp.where(a_s > 0.0, s, here)
                moved = here - (f_e - f_w) - lat
                adv[i, jt, t, :, pl.ds(0, width)] = moved
                parts.append(moved)
            tally(i, jt, parts)

    def gather(low, count, jt, tall):
        block = (pl.ds(low, count), pl.ds(jt, tall))
        level[block] = jnp.broadcast_to(
            jnp.sum(part[block], axis=3, keepdims=True) * scale, (count, tall, 8, LANES)
        )

    def weigh(i, jts):
        for jt in jts:
            parts = []
            spot = pl.ds(8 * jt, 8)
            energy = level[i, jt]
            for t in range(pieces):
                width = width_of(t)
                cut = (slice(None), slice(0, width))
                moved = adv[i, jt, t, :, pl.ds(0, width)]
                blow = wxs[i, spot, :][cut] * table(2, t) + wys[i, spot, :][cut] * table(3, t)
                gain = jnp.maximum(blow, 0.0) + seas[i, spot, :][cut]
                loss = table(4, t) * moved
                damp = 1.0 + energy[cut] * loss
                square = damp * damp
                inverse = pl.reciprocal(square, approx=True)
                inverse = inverse * (2.0 - square * inverse)
                weighted = inc[i, spot, pl.ds(t * LANES, width)] * gain * inverse
                put(ss_main, ss_tail, i + 1, t, PAD + 8 * jt, weighted)
                parts.append(weighted * loss * moved)
            tally(i, jt, parts)

    def settle(i, jts):
        for jt in jts:
            line = PAD + 8 * jt
            pull = level[i, jt]
            for t in range(pieces):
                value = at(ss_main, ss_tail, i + 1, t, line) - pull[:, : width_of(t)]
                put(ss_main, ss_tail, i + 1, t, line, value)

    def source(low, count, jts):
        jts = list(jts)
        prime(low, jts)
        spans = [(jts[0], len(jts))] if jts[-1] - jts[0] == len(jts) - 1 else [(jt, 1) for jt in jts]
        for step in (advect, weigh, settle):
            if count == 1:
                step(low, jts)
            else:
                looped(low, low + count, lambda i: step(i, jts))
            if step is not settle:
                for jt, tall in spans:
                    gather(low, count, jt, tall)

    def transport(cells):
        for i, jt in cells:
            for t in range(pieces):
                a_e, a_w, a_n, a_s = faces(i, jt, t)
                here, e, w, n, s = around(ss_main, ss_tail, i, jt, t)
                lon = jnp.maximum(a_e, 0.0) * (e - here) + jnp.minimum(a_w, 0.0) * (here - w)
                lat = jnp.maximum(a_n, 0.0) * (n - here) + jnp.minimum(a_s, 0.0) * (here - s)
                out[i, pl.ds(8 * jt, 8), pl.ds(t * LANES, width_of(t))] = here + lon + lat

    def looped(low, high, run):
        def step(i, carry):
            run(i)
            return carry

        lax.fori_loop(low, high, step, 0)

    middle = range(1, tiles - 1)
    everywhere = range(tiles)
    early = gy == ny // 2

    def inner_source():
        for copy in bulk:
            copy.wait()
        inc_load.wait()
        prepare()
        source(1, rows - 2, middle)

    for copy in small[:3] + last_row + first_row:
        copy.wait()
    pl.when(early)(inner_source)
    peers = 2 + lax.div(gy + ny - 1, ny) + lax.div(2 * ny - 2 - gy, ny)
    pl.semaphore_wait(barrier, peers)
    for side in sides:
        start(stat_copies, side)
    start(one, "east")
    start(one, "west")

    @pl.when(gy != ny // 2)
    def _():
        for copy in bulk:
            copy.wait()

    start(one, "north")
    start(one, "south")

    @pl.when(gy != ny // 2)
    def _():
        inc_load.wait()
        prepare()
        source(1, rows - 2, middle)

    for side in sides:
        wait_recv(stat_copies, side)
    prepare_edges()
    for side in sides:
        wait_recv(one, side)
    source(rows - 1, 1, everywhere)
    start(two, "east")
    source(0, 1, everywhere)
    start(two, "west")
    source(1, rows - 2, (0, tiles - 1))
    start(two, "north")
    start(two, "south")
    looped(1, rows - 1, lambda i: transport([(i, jt) for jt in middle]))
    for side in sides:
        wait_recv(two, side)
    looped(1, rows - 1, lambda i: transport([(i, 0), (i, tiles - 1)]))
    transport([(0, jt) for jt in everywhere])
    transport([(rows - 1, jt) for jt in everywhere])
    for group in (stat_copies, one, two):
        for side in sides:
            wait_send(group, side)


def body(
    spectrum,
    adjoint_in,
    current_x,
    current_y,
    wind_x,
    wind_y,
    land_mask,
    ice_mask,
    group_speed,
    growth_rate,
    dissipation,
):
    rows, cols, bins = spectrum.shape
    freqs = group_speed.shape[0]
    angles = np.float32(2.0 * math.pi / DIRS) * (np.arange(DIRS, dtype=np.float32) + np.float32(0.5))
    wave = np.zeros((8, -(-bins // LANES) * LANES), np.float32)
    wave[0, :bins] = np.repeat(np.cos(angles), freqs)
    wave[1, :bins] = np.repeat(np.sin(angles), freqs)
    mains = bins // LANES
    tail = bins - mains * LANES
    tall = cols + 2 * PAD
    f32 = jnp.float32
    any_space = pl.BlockSpec(memory_space=pl.ANY)
    return pl.pallas_call(
        kernel,
        out_shape=pltpu.VMEM((rows, cols, bins), f32),
        in_specs=[any_space] * 12,
        out_specs=pl.BlockSpec(memory_space=pltpu.VMEM),
        scratch_shapes=[
            pltpu.VMEM((rows + 2, mains, tall, LANES), f32),
            pltpu.VMEM((rows + 2, tall, tail), f32),
            pltpu.VMEM((rows + 2, mains, tall, LANES), f32),
            pltpu.VMEM((rows + 2, tall, tail), f32),
            pltpu.VMEM((rows, cols, bins), f32),
            pltpu.VMEM((rows, cols // 8, mains + 1, 8, LANES), f32),
            pltpu.VMEM((rows + 1, cols, LANES), f32),
            pltpu.VMEM((rows + 1, cols, LANES), f32),
            pltpu.VMEM((rows, tall, LANES), f32),
            pltpu.VMEM((rows, tall, LANES), f32),
            pltpu.VMEM((rows, cols, LANES), f32),
            pltpu.VMEM((rows, cols, LANES), f32),
            pltpu.VMEM((rows, cols, LANES), f32),
            pltpu.VMEM((cols // 8, mains + 1, 8, LANES), f32),
            pltpu.VMEM((rows, cols // 8, 8, LANES), f32),
            pltpu.VMEM((rows, cols // 8, 8, LANES), f32),
            pltpu.VMEM((3, 1, freqs), f32),
            pltpu.VMEM(wave.shape, f32),
            pltpu.VMEM((8, LANES), f32),
            pltpu.VMEM((5 * (mains + 1), 8, LANES), f32),
            pltpu.VMEM((4, rows, cols), f32),
            pltpu.VMEM((2, rows, cols), jnp.int32),
            pltpu.VMEM((4, rows, cols), f32),
            pltpu.VMEM((4, rows, cols), jnp.int32),
            pltpu.VMEM((32, LANES), f32),
            pltpu.SemaphoreType.DMA((3 * (mains + 1) + 11,)),
            pltpu.SemaphoreType.DMA((24,)),
            pltpu.SemaphoreType.DMA((24,)),
        ],
        compiler_params=pltpu.CompilerParams(
            collective_id=0, has_side_effects=True, vmem_limit_bytes=50 * 1024 * 1024
        ),
    )(
        spectrum,
        adjoint_in,
        current_x,
        current_y,
        wind_x,
        wind_y,
        land_mask,
        ice_mask,
        group_speed.reshape(1, freqs),
        growth_rate.reshape(1, freqs),
        dissipation.reshape(1, freqs),
        jnp.asarray(wave),
    )


def solution(mesh):
    cells = P("gx", "gy", None)
    placed = (cells, cells) + (P("gx", "gy"),) * 6 + (P(),) * 3
    return jax.shard_map(body, mesh=mesh, in_specs=placed, out_specs=cells, check_vma=False)
```

```python
import math

import jax
import jax.numpy as jnp
import numpy as np
from jax import lax
from jax.experimental import pallas as pl
from jax.experimental.pallas import tpu as pltpu
from jax.sharding import PartitionSpec as P

DIRS = 36
LANES = 128
PAD = 8
MESH = pl.DeviceIdType.MESH


def kernel(
    spec_hbm,
    adj_hbm,
    cx_hbm,
    cy_hbm,
    wx_hbm,
    wy_hbm,
    land_hbm,
    ice_hbm,
    speed_hbm,
    growth_hbm,
    loss_hbm,
    wave_hbm,
    out,
    sp_main,
    sp_tail,
    ss_main,
    ss_tail,
    inc,
    adv,
    oxs,
    pxs,
    oys,
    pys,
    wxs,
    wys,
    seas,
    fx,
    part,
    level,
    col,
    ci,
    sc,
    dc,
    par_in,
    wave,
    par,
    tab,
    stat_f,
    stat_i,
    nb_f,
    nb_i,
    ext,
    load_sem,
    send_sem,
    recv_sem,
):
    rows, cols, bins = spec_hbm.shape
    mains = bins // LANES
    tail = bins - mains * LANES
    tiles = cols // 8
    pieces = mains + 1
    gx = lax.axis_index("gx")
    gy = lax.axis_index("gy")
    nx = lax.axis_size("gx")
    ny = lax.axis_size("gy")
    east = lax.rem(gx + 1, nx)
    west = lax.rem(gx + nx - 1, nx)
    has_north = gy < ny - 1
    has_south = gy > 0
    body = pl.ds(PAD, cols)

    def local(src, dst, k):
        return pltpu.make_async_copy(src, dst, load_sem.at[k])

    def loads_of(low, count, base):
        copies = []
        for t in range(pieces):
            src_lanes = pl.ds(t * LANES, LANES if t < mains else tail)
            src = spec_hbm.at[pl.ds(low, count), :, src_lanes]
            if t < mains:
                dst = sp_main.at[pl.ds(low + 1, count), t, body, :]
            else:
                dst = sp_tail.at[pl.ds(low + 1, count), body, :]
            copies.append(local(src, dst, base + t))
        return copies

    first_row = loads_of(0, 1, 0)
    last_row = loads_of(rows - 1, 1, pieces)
    bulk = loads_of(1, rows - 2, 2 * pieces)
    base = 3 * pieces
    small = [
        local(land_hbm, stat_i.at[0], base),
        local(cx_hbm, stat_f.at[0], base + 1),
        local(cy_hbm, stat_f.at[1], base + 2),
        local(wx_hbm, stat_f.at[2], base + 3),
        local(wy_hbm, stat_f.at[3], base + 4),
        local(ice_hbm, stat_i.at[1], base + 5),
        local(speed_hbm, par_in.at[0], base + 6),
        local(growth_hbm, par_in.at[1], base + 7),
        local(loss_hbm, par_in.at[2], base + 8),
        local(wave_hbm, wave, base + 9),
    ]
    inc_load = local(adj_hbm, inc, base + 10)
    col_loads = [
        local(spec_hbm.at[:, j, :], col.at[k], base + 10 + k)
        for k, j in ((1, 0), (4, cols - 1), (2, 1), (3, cols - 2))
    ]
    ci_loads = [
        local(adj_hbm.at[:, j, :], ci.at[k], base + 15 + k) for k, j in ((0, 0), (1, cols - 1))
    ]
    for copy in small + last_row + first_row + col_loads + bulk + ci_loads + [inc_load]:
        copy.start()

    barrier = pltpu.get_barrier_semaphore()
    for target in (east, west):
        pl.semaphore_signal(barrier, inc=1, device_id={"gx": target}, device_id_type=MESH)

    @pl.when(has_north)
    def _():
        pl.semaphore_signal(barrier, inc=1, device_id={"gy": gy + 1}, device_id_type=MESH)

    @pl.when(has_south)
    def _():
        pl.semaphore_signal(barrier, inc=1, device_id={"gy": gy - 1}, device_id_type=MESH)

    def remote(src, dst, k, device):
        return pltpu.make_async_remote_copy(
            src_ref=src,
            dst_ref=dst,
            send_sem=send_sem.at[k],
            recv_sem=recv_sem.at[k],
            device_id=device,
            device_id_type=MESH,
        )

    to_east, to_west = {"gx": east}, {"gx": west}
    to_north, to_south = {"gy": gy + 1}, {"gy": gy - 1}

    def edge(main, last, lines, k, side):
        if side == "north":
            return [remote(lines.at[lines.shape[0] - 2], lines.at[0], k, to_north)]
        if side == "south":
            return [remote(lines.at[1], lines.at[lines.shape[0] - 1], k, to_south)]
        src, dst, device = (rows, 0, to_east) if side == "east" else (1, rows + 1, to_west)
        return [
            remote(main.at[src, :, body, :], main.at[dst, :, body, :], k, device),
            remote(last.at[src, body, :], last.at[dst, body, :], k + 1, device),
        ]

    sides = ("east", "west", "north", "south")
    stat_copies = {}
    for s, (side, device, field) in enumerate(
        (("east", to_east, 0), ("west", to_west, 0), ("north", to_north, 1), ("south", to_south, 1))
    ):
        stat_copies[side] = [
            remote(stat_i.at[0], nb_i.at[s], 16 + 2 * s, device),
            remote(stat_f.at[field], nb_f.at[s], 17 + 2 * s, device),
        ]
    one = {side: edge(sp_main, sp_tail, col, 2 * s, side) for s, side in enumerate(sides)}
    two = {side: edge(ss_main, ss_tail, sc, 8 + 2 * s, side) for s, side in enumerate(sides)}

    sends_ok = {"east": None, "west": None, "north": has_north, "south": has_south}
    recvs_ok = {"east": None, "west": None, "north": has_south, "south": has_north}

    def guarded(condition, run):
        if condition is None:
            run()
        else:
            pl.when(condition)(run)

    def start(group, side):
        guarded(sends_ok[side], lambda: [copy.start() for copy in group[side]] and None)

    def wait_recv(group, side):
        guarded(recvs_ok[side], lambda: [copy.wait_recv() for copy in group[side]] and None)

    def wait_send(group, side):
        guarded(sends_ok[side], lambda: [copy.wait_send() for copy in group[side]] and None)

    lane = lax.broadcasted_iota(jnp.int32, (32, LANES), 1)
    row = lax.broadcasted_iota(jnp.int32, (32, LANES), 0)

    def widened(values):
        ext[...] = jnp.zeros((32, LANES), jnp.float32)
        ext[pl.ds(0, rows), pl.ds(0, cols)] = values
        return ext[...]

    def sea_of(mask):
        return (1 - mask).astype(jnp.float32)

    def around_lon(mine, from_east, from_west):
        up = pltpu.roll(widened(from_east), rows, 0)
        down = pltpu.roll(widened(from_west), 8, 0)
        return jnp.where(row == rows, up, jnp.where(row == 31, down, mine))

    def around_lat(mine, from_north, from_south):
        up = pltpu.roll(widened(from_north), cols, 1)
        down = pltpu.roll(widened(from_south), LANES - cols, 1)
        up = jnp.where(has_north, up, 0.0)
        down = jnp.where(has_south, down, 0.0)
        return jnp.where(lane == cols, up, jnp.where(lane == LANES - 1, down, mine))

    def spread(field, places):
        turned = jnp.transpose(field)
        for dst, spot, column, r in places:
            count = column.stop - column.start
            dst[spot] = jnp.broadcast_to(turned[column, r : r + 1], (count, LANES))

    inside = slice(0, cols)
    inside_at = pl.ds(PAD, cols)

    def lon_faces(sea_lon, drift_lon):
        opened = sea_lon * pltpu.roll(sea_lon, 31, 0)
        return opened, opened * (0.5 * (drift_lon + pltpu.roll(drift_lon, 31, 0)))

    def lat_faces(sea_lat, drift_lat):
        opened = sea_lat * pltpu.roll(sea_lat, LANES - 1, 1)
        return opened, opened * (0.5 * (drift_lat + pltpu.roll(drift_lat, LANES - 1, 1)))

    def prepare():
        for copy in small[3:]:
            copy.wait()
        par[...] = jnp.zeros((8, LANES), jnp.float32)
        freqs = speed_hbm.shape[1]
        for k in range(3):
            par[pl.ds(k, 1), pl.ds(0, freqs)] = par_in[k]
        per_freq = par[...]
        bin_lane = lax.broadcasted_iota(jnp.int32, (8, LANES), 1)
        for t in range(pieces):
            freq = lax.rem(bin_lane + t * LANES, freqs)
            picked = jnp.take_along_axis(per_freq, freq, axis=1)
            full = (8, LANES)
            speed = jnp.broadcast_to(picked[0:1], full)
            growth = jnp.broadcast_to(picked[1:2], full)
            cosine = jnp.broadcast_to(wave[pl.ds(0, 1), pl.ds(t * LANES, LANES)], full)
            sine = jnp.broadcast_to(wave[pl.ds(1, 1), pl.ds(t * LANES, LANES)], full)
            tab[t] = speed * cosine
            tab[pieces + t] = speed * sine
            tab[2 * pieces + t] = growth * cosine
            tab[3 * pieces + t] = growth * sine
            tab[4 * pieces + t] = jnp.broadcast_to(picked[2:3], full)
        sea = widened(sea_of(stat_i[0]))
        wet = widened(sea_of(stat_i[1])) * sea
        every = range(rows)
        spread(sea, [(seas, r, inside, r) for r in every])
        spread(widened(stat_f[2]) * wet, [(wxs, r, inside, r) for r in every])
        spread(widened(stat_f[3]) * wet, [(wys, r, inside, r) for r in every])
        for field, dst in zip(lon_faces(sea, widened(stat_f[0])), (oxs, pxs)):
            spread(field, [(dst, r + 1, inside, r) for r in range(rows - 1)])
        for field, dst in zip(lat_faces(sea, widened(stat_f[1])), (oys, pys)):
            spread(field, [(dst, (r, inside_at), inside, r) for r in every])
            for r in every:
                dst[r, pl.ds(0, PAD), :] = jnp.zeros((PAD, LANES), jnp.float32)

    def prepare_edges():
        sea = widened(sea_of(stat_i[0]))
        sea_lon = around_lon(sea, sea_of(nb_i[1]), sea_of(nb_i[0]))
        sea_lat = around_lat(sea, sea_of(nb_i[3]), sea_of(nb_i[2]))
        drift_lon = around_lon(widened(stat_f[0]), nb_f[1], nb_f[0])
        drift_lat = around_lat(widened(stat_f[1]), nb_f[3], nb_f[2])
        for field, dst in zip(lon_faces(sea_lon, drift_lon), (oxs, pxs)):
            spread(field, [(dst, 0, inside, 31), (dst, rows, inside, rows - 1)])
        wet = widened(sea_of(stat_i[1])) * sea
        lon = lon_faces(sea_lon, drift_lon)
        lat = lat_faces(sea_lat, drift_lat)
        fields = list(lon) + [pltpu.roll(field, 1, 0) for field in lon]
        fields += list(lat) + [pltpu.roll(field, 1, 1) for field in lat]
        fields += [widened(stat_f[2]) * wet, widened(stat_f[3]) * wet, sea]
        for k, j in enumerate((0, cols - 1)):
            for m, field in enumerate(fields):
                dc[k, m] = jnp.broadcast_to(field[0:rows, j : j + 1], (rows, LANES))

    def width_of(t):
        return LANES if t < mains else tail

    def at(main, last, r, t, line):
        if t < mains:
            return main[r, t, pl.ds(line, 8), :]
        return last[r, pl.ds(line, 8), :]

    def put(main, last, r, t, line, value):
        if t < mains:
            main[r, t, pl.ds(line, 8), :] = value
        else:
            last[r, pl.ds(line, 8), :] = value

    def table(k, t):
        return tab[k * pieces + t, :, pl.ds(0, width_of(t))]

    def faces(i, jt, t):
        cut = (slice(None), slice(0, width_of(t)))
        line = PAD + 8 * jt
        cos_speed, sin_speed = table(0, t), table(1, t)
        spot = pl.ds(8 * jt, 8)
        a_e = oxs[i + 1, spot, :][cut] * cos_speed + pxs[i + 1, spot, :][cut]
        a_w = oxs[i, spot, :][cut] * cos_speed + pxs[i, spot, :][cut]
        a_n = oys[i, pl.ds(line, 8), :][cut] * sin_speed + pys[i, pl.ds(line, 8), :][cut]
        a_s = oys[i, pl.ds(line - 1, 8), :][cut] * sin_speed + pys[i, pl.ds(line - 1, 8), :][cut]
        return a_e, a_w, a_n, a_s

    scale = 1.0 / bins

    def lon_flux(i, jt, t):
        cut = (slice(None), slice(0, width_of(t)))
        spot = pl.ds(8 * jt, 8)
        line = PAD + 8 * jt
        pace = oxs[i + 1, spot, :][cut] * table(0, t) + pxs[i + 1, spot, :][cut]
        here, e = at(sp_main, sp_tail, i + 1, t, line), at(sp_main, sp_tail, i + 2, t, line)
        return pace * jnp.where(pace > 0.0, here, e)

    def tally(i, jt, parts):
        whole = parts[0]
        for more in parts[1:mains]:
            whole = whole + more
        part[i, jt] = whole
        part[i, jt, :, pl.ds(0, tail)] = whole[:, :tail] + parts[mains]

    def prime(i, jts):
        for jt in jts:
            for t in range(pieces):
                fx[jt, t, :, pl.ds(0, width_of(t))] = lon_flux(i - 1, jt, t)

    def advect(i, jts):
        for jt in jts:
            parts = []
            spot = pl.ds(PAD + 8 * jt, 8)
            under = pl.ds(PAD + 8 * jt - 1, 8)
            for t in range(pieces):
                width = width_of(t)
                cut = (slice(None), slice(0, width))
                sin_speed = table(1, t)
                a_n = oys[i, spot, :][cut] * sin_speed + pys[i, spot, :][cut]
                a_s = oys[i, under, :][cut] * sin_speed + pys[i, under, :][cut]
                line = PAD + 8 * jt
                here = at(sp_main, sp_tail, i + 1, t, line)
                n = at(sp_main, sp_tail, i + 1, t, line + 1)
                s = at(sp_main, sp_tail, i + 1, t, line - 1)
                f_w = fx[jt, t, :, pl.ds(0, width)]
                f_e = lon_flux(i, jt, t)
                fx[jt, t, :, pl.ds(0, width)] = f_e
                lat = a_n * jnp.where(a_n < 0.0, n, here) - a_s * jnp.where(a_s > 0.0, s, here)
                moved = here - (f_e - f_w) - lat
                adv[i, jt, t, :, pl.ds(0, width)] = moved
                parts.append(moved)
            tally(i, jt, parts)

    def gather(low, count, jt, tall):
        block = (pl.ds(low, count), pl.ds(jt, tall))
        level[block] = jnp.broadcast_to(
            jnp.sum(part[block], axis=3, keepdims=True) * scale, (count, tall, 8, LANES)
        )

    def weigh(i, jts):
        for jt in jts:
            parts = []
            spot = pl.ds(8 * jt, 8)
            energy = level[i, jt]
            for t in range(pieces):
                width = width_of(t)
                cut = (slice(None), slice(0, width))
                moved = adv[i, jt, t, :, pl.ds(0, width)]
                blow = wxs[i, spot, :][cut] * table(2, t) + wys[i, spot, :][cut] * table(3, t)
                gain = jnp.maximum(blow, 0.0) + seas[i, spot, :][cut]
                loss = table(4, t) * moved
                damp = 1.0 + energy[cut] * loss
                square = damp * damp
                inverse = pl.reciprocal(square, approx=True)
                inverse = inverse * (2.0 - square * inverse)
                weighted = inc[i, spot, pl.ds(t * LANES, width)] * gain * inverse
                put(ss_main, ss_tail, i + 1, t, PAD + 8 * jt, weighted)
                parts.append(weighted * loss * moved)
            tally(i, jt, parts)

    def settle(i, jts):
        for jt in jts:
            line = PAD + 8 * jt
            pull = level[i, jt]
            for t in range(pieces):
                value = at(ss_main, ss_tail, i + 1, t, line) - pull[:, : width_of(t)]
                put(ss_main, ss_tail, i + 1, t, line, value)

    def source(low, count, jts):
        jts = list(jts)
        prime(low, jts)
        spans = [(jts[0], len(jts))] if jts[-1] - jts[0] == len(jts) - 1 else [(jt, 1) for jt in jts]
        for step in (advect, weigh, settle):
            if count == 1:
                step(low, jts)
            else:
                looped(low, low + count, lambda i: step(i, jts))
            if step is not settle:
                for jt, tall in spans:
                    gather(low, count, jt, tall)

    row_at = lax.broadcasted_iota(jnp.int32, (rows, LANES), 0)

    def line(main, last, r, t, place):
        if t < mains:
            return main.at[r, t, pl.ds(place, 1), :]
        return last.at[r, pl.ds(place, 1), :]

    def lanes_of(t):
        return pl.ds(t * LANES, width_of(t))

    def lane_sum(parts):
        whole = parts[0]
        for more in parts[1:mains]:
            whole = whole + more
        return jnp.sum(whole, axis=1, keepdims=True) + jnp.sum(parts[mains], axis=1, keepdims=True)

    def wide_table(k, t):
        return jnp.broadcast_to(tab[k * pieces + t, pl.ds(0, 1), pl.ds(0, width_of(t))], (rows, width_of(t)))

    def edge_columns():
        ends = (0, 1)
        places = (PAD, PAD + cols - 1)
        sums = [[], []]
        for k in ends:
            here_at, n_at, s_at = ((1, 2, 0), (4, 5, 3))[k]
            for t in range(pieces):
                width = width_of(t)
                coef = [dc[k, m][:, :width] for m in range(8)]
                cos_speed, sin_speed = wide_table(0, t), wide_table(1, t)
                here = col[here_at, :, lanes_of(t)]
                n, s = col[n_at, :, lanes_of(t)], col[s_at, :, lanes_of(t)]
                e_end = line(sp_main, sp_tail, rows + 1, t, places[k])[...]
                w_end = line(sp_main, sp_tail, 0, t, places[k])[...]
                at_row = row_at[:, :width]
                e = jnp.where(at_row == rows - 1, e_end, pltpu.roll(here, rows - 1, 0))
                w = jnp.where(at_row == 0, w_end, pltpu.roll(here, 1, 0))
                a_e = coef[0] * cos_speed + coef[1]
                a_w = coef[2] * cos_speed + coef[3]
                a_n = coef[4] * sin_speed + coef[5]
                a_s = coef[6] * sin_speed + coef[7]
                lon = a_e * jnp.where(a_e < 0.0, e, here) - a_w * jnp.where(a_w > 0.0, w, here)
                lat = a_n * jnp.where(a_n < 0.0, n, here) - a_s * jnp.where(a_s > 0.0, s, here)
                moved = here - lon - lat
                sc[1 + k, :, lanes_of(t)] = moved
                sums[k].append(moved)
        energies = [lane_sum(sums[k]) * scale for k in ends]
        pulls = [[], []]
        for k in ends:
            energy = jnp.broadcast_to(energies[k], (rows, LANES))
            for t in range(pieces):
                width = width_of(t)
                wind_x, wind_y, open_sea = [dc[k, m][:, :width] for m in range(8, 11)]
                moved = sc[1 + k, :, lanes_of(t)]
                blow = wind_x * wide_table(2, t) + wind_y * wide_table(3, t)
                gain = jnp.maximum(blow, 0.0) + open_sea
                loss = wide_table(4, t) * moved
                damp = 1.0 + energy[:, :width] * loss
                square = damp * damp
                inverse = pl.reciprocal(square, approx=True)
                inverse = inverse * (2.0 - square * inverse)
                weighted = ci[k, :, lanes_of(t)] * gain * inverse
                sc[1 + k, :, lanes_of(t)] = weighted
                pulls[k].append(weighted * loss * moved)
        ends_pull = [lane_sum(pulls[k]) * scale for k in ends]
        for k in ends:
            pull = jnp.broadcast_to(ends_pull[k], (rows, LANES))
            for t in range(pieces):
                sc[1 + k, :, lanes_of(t)] = sc[1 + k, :, lanes_of(t)] - pull[:, : width_of(t)]

    def insert_columns(which):
        for i in which:
            for k, place in enumerate((PAD, PAD + cols - 1)):
                for t in range(pieces):
                    target = line(ss_main, ss_tail, i + 1, t, place)
                    target[...] = sc[1 + k, pl.ds(i, 1), lanes_of(t)]

    def transport(cells, skip_e=False, skip_w=False):
        for i, jt in cells:
            for t in range(pieces):
                a_e, a_w, a_n, a_s = faces(i, jt, t)
                place = PAD + 8 * jt
                here = at(ss_main, ss_tail, i + 1, t, place)
                n = at(ss_main, ss_tail, i + 1, t, place + 1)
                s = at(ss_main, ss_tail, i + 1, t, place - 1)
                total = here
                if not skip_e:
                    e = at(ss_main, ss_tail, i + 2, t, place)
                    total = total + jnp.maximum(a_e, 0.0) * (e - here)
                if not skip_w:
                    w = at(ss_main, ss_tail, i, t, place)
                    total = total + jnp.minimum(a_w, 0.0) * (here - w)
                if jt == tiles - 1:
                    total = total + jnp.where(a_n > 0.0, a_n * (n - here), 0.0)
                else:
                    total = total + jnp.maximum(a_n, 0.0) * (n - here)
                if jt == 0:
                    total = total + jnp.where(a_s < 0.0, a_s * (here - s), 0.0)
                else:
                    total = total + jnp.minimum(a_s, 0.0) * (here - s)
                out[i, pl.ds(8 * jt, 8), lanes_of(t)] = total

    def finish_row(i):
        for jt in range(tiles):
            spot = pl.ds(8 * jt, 8)
            for t in range(pieces):
                cut = (slice(None), slice(0, width_of(t)))
                here = at(ss_main, ss_tail, i + 1, t, PAD + 8 * jt)
                if i == 0:
                    a_w = oxs[0, spot, :][cut] * table(0, t) + pxs[0, spot, :][cut]
                    term = jnp.minimum(a_w, 0.0) * (here - at(ss_main, ss_tail, 0, t, PAD + 8 * jt))
                else:
                    a_e = oxs[rows, spot, :][cut] * table(0, t) + pxs[rows, spot, :][cut]
                    far = at(ss_main, ss_tail, rows + 1, t, PAD + 8 * jt)
                    term = jnp.maximum(a_e, 0.0) * (far - here)
                out[i, spot, lanes_of(t)] = out[i, spot, lanes_of(t)] + term

    def finish_column(k):
        for t in range(pieces):
            width = width_of(t)
            here = sc[1 + k, :, lanes_of(t)]
            if k == 0:
                a_s = dc[0, 6][:, :width] * wide_table(1, t) + dc[0, 7][:, :width]
                term = jnp.where(a_s < 0.0, a_s * (here - sc[0, :, lanes_of(t)]), 0.0)
            else:
                a_n = dc[1, 4][:, :width] * wide_table(1, t) + dc[1, 5][:, :width]
                term = jnp.where(a_n > 0.0, a_n * (sc[3, :, lanes_of(t)] - here), 0.0)
            ci[k, :, lanes_of(t)] = term
        place = pl.ds(0 if k == 0 else cols - 1, 1)
        for i in range(rows):
            for t in range(pieces):
                term = ci[k, pl.ds(i, 1), lanes_of(t)]
                out[i, place, lanes_of(t)] = out[i, place, lanes_of(t)] + term

    def looped(low, high, run):
        def step(i, carry):
            run(i)
            return carry

        lax.fori_loop(low, high, step, 0)

    everywhere = range(tiles)
    early = gy == ny // 2
    late = gy != ny // 2
    first_part = (rows - 2) * 3 // 5

    def first_source():
        for copy in bulk:
            copy.wait()
        inc_load.wait()
        prepare()
        source(1, first_part, everywhere)

    def second_source():
        source(1 + first_part, rows - 2 - first_part, everywhere)

    for copy in small[:3] + last_row + first_row + col_loads[:2]:
        copy.wait()
    pl.when(early)(first_source)
    peers = 2 + lax.div(gy + ny - 1, ny) + lax.div(2 * ny - 2 - gy, ny)
    pl.semaphore_wait(barrier, peers)
    for side in sides:
        start(stat_copies, side)
    for side in ("north", "south", "east", "west"):
        start(one, side)
    pl.when(late)(first_source)
    pl.when(early)(second_source)
    for copy in col_loads[2:] + ci_loads:
        copy.wait()
    for side in sides:
        wait_recv(stat_copies, side)
    prepare_edges()
    for side in sides:
        wait_recv(one, side)
    edge_columns()
    start(two, "north")
    start(two, "south")
    source(rows - 1, 1, everywhere)
    source(0, 1, everywhere)
    insert_columns((0, rows - 1))
    start(two, "east")
    start(two, "west")
    pl.when(late)(second_source)
    insert_columns(range(1, rows - 1))
    looped(1, rows - 1, lambda i: transport([(i, jt) for jt in everywhere]))
    transport([(0, jt) for jt in everywhere], skip_w=True)
    transport([(rows - 1, jt) for jt in everywhere], skip_e=True)
    for side in ("west", "east"):
        wait_recv(two, side)
    finish_row(rows - 1)
    finish_row(0)
    wait_recv(two, "south")
    finish_column(1)
    wait_recv(two, "north")
    finish_column(0)
    for group in (stat_copies, one, two):
        for side in sides:
            wait_send(group, side)


def body(
    spectrum,
    adjoint_in,
    current_x,
    current_y,
    wind_x,
    wind_y,
    land_mask,
    ice_mask,
    group_speed,
    growth_rate,
    dissipation,
):
    rows, cols, bins = spectrum.shape
    freqs = group_speed.shape[0]
    angles = np.float32(2.0 * math.pi / DIRS) * (np.arange(DIRS, dtype=np.float32) + np.float32(0.5))
    wave = np.zeros((8, -(-bins // LANES) * LANES), np.float32)
    wave[0, :bins] = np.repeat(np.cos(angles), freqs)
    wave[1, :bins] = np.repeat(np.sin(angles), freqs)
    mains = bins // LANES
    tail = bins - mains * LANES
    tall = cols + 2 * PAD
    f32 = jnp.float32
    any_space = pl.BlockSpec(memory_space=pl.ANY)
    return pl.pallas_call(
        kernel,
        out_shape=pltpu.VMEM((rows, cols, bins), f32),
        in_specs=[any_space] * 12,
        out_specs=pl.BlockSpec(memory_space=pltpu.VMEM),
        scratch_shapes=[
            pltpu.VMEM((rows + 2, mains, tall, LANES), f32),
            pltpu.VMEM((rows + 2, tall, tail), f32),
            pltpu.VMEM((rows + 2, mains, tall, LANES), f32),
            pltpu.VMEM((rows + 2, tall, tail), f32),
            pltpu.VMEM((rows, cols, bins), f32),
            pltpu.VMEM((rows, cols // 8, mains + 1, 8, LANES), f32),
            pltpu.VMEM((rows + 1, cols, LANES), f32),
            pltpu.VMEM((rows + 1, cols, LANES), f32),
            pltpu.VMEM((rows, tall, LANES), f32),
            pltpu.VMEM((rows, tall, LANES), f32),
            pltpu.VMEM((rows, cols, LANES), f32),
            pltpu.VMEM((rows, cols, LANES), f32),
            pltpu.VMEM((rows, cols, LANES), f32),
            pltpu.VMEM((cols // 8, mains + 1, 8, LANES), f32),
            pltpu.VMEM((rows, cols // 8, 8, LANES), f32),
            pltpu.VMEM((rows, cols // 8, 8, LANES), f32),
            pltpu.VMEM((6, rows, bins), f32),
            pltpu.VMEM((2, rows, bins), f32),
            pltpu.VMEM((4, rows, bins), f32),
            pltpu.VMEM((2, 11, rows, LANES), f32),
            pltpu.VMEM((3, 1, freqs), f32),
            pltpu.VMEM(wave.shape, f32),
            pltpu.VMEM((8, LANES), f32),
            pltpu.VMEM((5 * (mains + 1), 8, LANES), f32),
            pltpu.VMEM((4, rows, cols), f32),
            pltpu.VMEM((2, rows, cols), jnp.int32),
            pltpu.VMEM((4, rows, cols), f32),
            pltpu.VMEM((4, rows, cols), jnp.int32),
            pltpu.VMEM((32, LANES), f32),
            pltpu.SemaphoreType.DMA((3 * (mains + 1) + 17,)),
            pltpu.SemaphoreType.DMA((24,)),
            pltpu.SemaphoreType.DMA((24,)),
        ],
        compiler_params=pltpu.CompilerParams(
            collective_id=0, has_side_effects=True, vmem_limit_bytes=50 * 1024 * 1024
        ),
    )(
        spectrum,
        adjoint_in,
        current_x,
        current_y,
        wind_x,
        wind_y,
        land_mask,
        ice_mask,
        group_speed.reshape(1, freqs),
        growth_rate.reshape(1, freqs),
        dissipation.reshape(1, freqs),
        jnp.asarray(wave),
    )


def solution(mesh):
    cells = P("gx", "gy", None)
    placed = (cells, cells) + (P("gx", "gy"),) * 6 + (P(),) * 3
    return jax.shard_map(body, mesh=mesh, in_specs=placed, out_specs=cells, check_vma=False)
```

```python
import math

import jax
import jax.numpy as jnp
import numpy as np
from jax import lax
from jax.experimental import pallas as pl
from jax.experimental.pallas import tpu as pltpu
from jax.sharding import PartitionSpec as P

DIRS = 36
LANES = 128
LEAST_SPEED = 0.1
MOST_CURRENT = 0.08
PAD = 8
MESH = pl.DeviceIdType.MESH


def directions(bins):
    angles = np.float32(2.0 * math.pi / DIRS) * (np.arange(DIRS, dtype=np.float32) + np.float32(0.5))
    per_dir = bins // DIRS
    return np.repeat(np.cos(angles), per_dir), np.repeat(np.sin(angles), per_dir)


def one_way(heading):
    sure = 1.001 * MOST_CURRENT / LEAST_SPEED
    starts = range(0, heading.size, LANES)
    forward = [t for t, b in enumerate(starts) if np.all(heading[b : b + LANES] > sure)]
    backward = [t for t, b in enumerate(starts) if np.all(heading[b : b + LANES] < -sure)]
    return forward, backward


def kernel(
    spec_hbm,
    adj_hbm,
    cx_hbm,
    cy_hbm,
    wx_hbm,
    wy_hbm,
    land_hbm,
    ice_hbm,
    speed_hbm,
    growth_hbm,
    loss_hbm,
    wave_hbm,
    out,
    sp_main,
    sp_tail,
    ss_main,
    ss_tail,
    inc,
    adv,
    oxs,
    pxs,
    oys,
    pys,
    wxs,
    wys,
    seas,
    fx,
    part,
    level,
    col,
    ci,
    sc,
    dc,
    par_in,
    wave,
    par,
    tab,
    stat_f,
    stat_i,
    nb_f,
    nb_i,
    ext,
    load_sem,
    send_sem,
    recv_sem,
):
    rows, cols, bins = spec_hbm.shape
    mains = bins // LANES
    tail = bins - mains * LANES
    tiles = cols // 8
    pieces = mains + 1
    gx = lax.axis_index("gx")
    gy = lax.axis_index("gy")
    nx = lax.axis_size("gx")
    ny = lax.axis_size("gy")
    east = lax.rem(gx + 1, nx)
    west = lax.rem(gx + nx - 1, nx)
    has_north = gy < ny - 1
    has_south = gy > 0
    body = pl.ds(PAD, cols)

    barrier = pltpu.get_barrier_semaphore()
    for target in (east, west):
        pl.semaphore_signal(barrier, inc=1, device_id={"gx": target}, device_id_type=MESH)

    @pl.when(has_north)
    def _():
        pl.semaphore_signal(barrier, inc=1, device_id={"gy": gy + 1}, device_id_type=MESH)

    @pl.when(has_south)
    def _():
        pl.semaphore_signal(barrier, inc=1, device_id={"gy": gy - 1}, device_id_type=MESH)

    def local(src, dst, k):
        return pltpu.make_async_copy(src, dst, load_sem.at[k])

    def loads_of(low, count, base):
        copies = []
        for t in range(pieces):
            src_lanes = pl.ds(t * LANES, LANES if t < mains else tail)
            src = spec_hbm.at[pl.ds(low, count), :, src_lanes]
            if t < mains:
                dst = sp_main.at[pl.ds(low + 1, count), t, body, :]
            else:
                dst = sp_tail.at[pl.ds(low + 1, count), body, :]
            copies.append(local(src, dst, base + t))
        return copies

    first_row = loads_of(0, 1, 0)
    last_row = loads_of(rows - 1, 1, pieces)
    bulk = loads_of(1, rows - 2, 2 * pieces)
    base = 3 * pieces
    small = [
        local(land_hbm, stat_i.at[0], base),
        local(cx_hbm, stat_f.at[0], base + 1),
        local(cy_hbm, stat_f.at[1], base + 2),
        local(wx_hbm, stat_f.at[2], base + 3),
        local(wy_hbm, stat_f.at[3], base + 4),
        local(ice_hbm, stat_i.at[1], base + 5),
        local(speed_hbm, par_in.at[0], base + 6),
        local(growth_hbm, par_in.at[1], base + 7),
        local(loss_hbm, par_in.at[2], base + 8),
        local(wave_hbm, wave, base + 9),
    ]
    inc_load = local(adj_hbm, inc, base + 10)
    col_loads = [
        local(spec_hbm.at[:, j, :], col.at[k], base + 10 + k)
        for k, j in ((1, 0), (4, cols - 1), (2, 1), (3, cols - 2))
    ]
    ci_loads = [
        local(adj_hbm.at[:, j, :], ci.at[k], base + 15 + k) for k, j in ((0, 0), (1, cols - 1))
    ]
    for copy in small + last_row + first_row + col_loads + bulk + ci_loads + [inc_load]:
        copy.start()

    def remote(src, dst, k, device):
        return pltpu.make_async_remote_copy(
            src_ref=src,
            dst_ref=dst,
            send_sem=send_sem.at[k],
            recv_sem=recv_sem.at[k],
            device_id=device,
            device_id_type=MESH,
        )

    to_east, to_west = {"gx": east}, {"gx": west}
    to_north, to_south = {"gy": gy + 1}, {"gy": gy - 1}

    used = iter(range(24))

    def runs(skip):
        spans, low = [], 0
        for t in sorted(skip) + [pieces]:
            if t > low:
                spans.append((low, t))
            low = t + 1
        return spans

    def edge(main, last, lines, side, skip):
        copies = []
        for low, high in runs(skip):
            if side in ("north", "south"):
                lanes = pl.ds(low * LANES, min(high * LANES, bins) - low * LANES)
                top = lines.shape[0] - 1
                src, dst, device = (top - 1, 0, to_north) if side == "north" else (1, top, to_south)
                copies.append(
                    remote(lines.at[src, :, lanes], lines.at[dst, :, lanes], next(used), device)
                )
                continue
            src, dst, device = (rows, 0, to_east) if side == "east" else (1, rows + 1, to_west)
            whole = pl.ds(low, min(high, mains) - low)
            copies.append(
                remote(main.at[src, whole, body, :], main.at[dst, whole, body, :], next(used), device)
            )
            if high == pieces:
                copies.append(
                    remote(last.at[src, body, :], last.at[dst, body, :], next(used), device)
                )
        return copies

    sides = ("east", "west", "north", "south")
    stat_copies = {}
    for s, (side, device, field) in enumerate(
        (("east", to_east, 0), ("west", to_west, 0), ("north", to_north, 1), ("south", to_south, 1))
    ):
        stat_copies[side] = [
            remote(stat_i.at[0], nb_i.at[s], next(used), device),
            remote(stat_f.at[field], nb_f.at[s], next(used), device),
        ]
    cosine, sine = directions(bins)
    (eastward, westward), (northward, southward) = one_way(cosine), one_way(sine)
    idle_one = {"east": westward, "west": eastward, "north": southward, "south": northward}
    idle_two = {"east": eastward, "west": westward, "north": northward, "south": southward}
    one = {side: edge(sp_main, sp_tail, col, side, idle_one[side]) for side in sides}
    two = {side: edge(ss_main, ss_tail, sc, side, idle_two[side]) for side in sides}

    sends_ok = {"east": None, "west": None, "north": has_north, "south": has_south}
    recvs_ok = {"east": None, "west": None, "north": has_south, "south": has_north}

    def guarded(condition, run):
        if condition is None:
            run()
        else:
            pl.when(condition)(run)

    def start(group, side):
        guarded(sends_ok[side], lambda: [copy.start() for copy in group[side]] and None)

    def wait_recv(group, side):
        guarded(recvs_ok[side], lambda: [copy.wait_recv() for copy in group[side]] and None)

    def wait_send(group, side):
        guarded(sends_ok[side], lambda: [copy.wait_send() for copy in group[side]] and None)

    lane = lax.broadcasted_iota(jnp.int32, (32, LANES), 1)
    row = lax.broadcasted_iota(jnp.int32, (32, LANES), 0)

    def widened(values):
        ext[...] = jnp.zeros((32, LANES), jnp.float32)
        ext[pl.ds(0, rows), pl.ds(0, cols)] = values
        return ext[...]

    def sea_of(mask):
        return (1 - mask).astype(jnp.float32)

    def around_lon(mine, from_east, from_west):
        up = pltpu.roll(widened(from_east), rows, 0)
        down = pltpu.roll(widened(from_west), 8, 0)
        return jnp.where(row == rows, up, jnp.where(row == 31, down, mine))

    def around_lat(mine, from_north, from_south):
        up = pltpu.roll(widened(from_north), cols, 1)
        down = pltpu.roll(widened(from_south), LANES - cols, 1)
        up = jnp.where(has_north, up, 0.0)
        down = jnp.where(has_south, down, 0.0)
        return jnp.where(lane == cols, up, jnp.where(lane == LANES - 1, down, mine))

    def spread(places):
        turned = {}
        for field, dst, spot, column, r in places:
            if id(field) not in turned:
                turned[id(field)] = jnp.transpose(field)
        for field, dst, spot, column, r in sorted(places, key=lambda place: place[4]):
            count = column.stop - column.start
            dst[spot] = jnp.broadcast_to(turned[id(field)][column, r : r + 1], (count, LANES))

    inside = slice(0, cols)
    inside_at = pl.ds(PAD, cols)

    def lon_faces(sea_lon, drift_lon):
        opened = sea_lon * pltpu.roll(sea_lon, 31, 0)
        return opened, opened * (0.5 * (drift_lon + pltpu.roll(drift_lon, 31, 0)))

    def lat_faces(sea_lat, drift_lat):
        opened = sea_lat * pltpu.roll(sea_lat, LANES - 1, 1)
        return opened, opened * (0.5 * (drift_lat + pltpu.roll(drift_lat, LANES - 1, 1)))

    def prepare():
        for copy in small[3:]:
            copy.wait()
        par[...] = jnp.zeros((8, LANES), jnp.float32)
        freqs = speed_hbm.shape[1]
        for k in range(3):
            par[pl.ds(k, 1), pl.ds(0, freqs)] = par_in[k]
        per_freq = par[...]
        bin_lane = lax.broadcasted_iota(jnp.int32, (8, LANES), 1)
        for t in range(pieces):
            freq = lax.rem(bin_lane + t * LANES, freqs)
            picked = jnp.take_along_axis(per_freq, freq, axis=1)
            full = (8, LANES)
            speed = jnp.broadcast_to(picked[0:1], full)
            growth = jnp.broadcast_to(picked[1:2], full)
            cosine = jnp.broadcast_to(wave[pl.ds(0, 1), pl.ds(t * LANES, LANES)], full)
            sine = jnp.broadcast_to(wave[pl.ds(1, 1), pl.ds(t * LANES, LANES)], full)
            tab[t] = speed * cosine
            tab[pieces + t] = speed * sine
            tab[2 * pieces + t] = growth * cosine
            tab[3 * pieces + t] = growth * sine
            tab[4 * pieces + t] = jnp.broadcast_to(picked[2:3], full)
        sea = widened(sea_of(stat_i[0]))
        wet = widened(sea_of(stat_i[1])) * sea
        every = range(rows)
        lon = lon_faces(sea, widened(stat_f[0]))
        lat = lat_faces(sea, widened(stat_f[1]))
        breeze = [widened(stat_f[2]) * wet, widened(stat_f[3]) * wet]
        places = []
        for r in every:
            places += [(field, dst, r, inside, r) for field, dst in zip(breeze + [sea], (wxs, wys, seas))]
            places += [(field, dst, (r, inside_at), inside, r) for field, dst in zip(lat, (oys, pys))]
            if r < rows - 1:
                places += [(field, dst, r + 1, inside, r) for field, dst in zip(lon, (oxs, pxs))]
        spread(places)
        for dst in (oys, pys):
            for r in every:
                dst[r, pl.ds(0, PAD), :] = jnp.zeros((PAD, LANES), jnp.float32)

    def prepare_edges():
        sea = widened(sea_of(stat_i[0]))
        sea_lon = around_lon(sea, sea_of(nb_i[1]), sea_of(nb_i[0]))
        sea_lat = around_lat(sea, sea_of(nb_i[3]), sea_of(nb_i[2]))
        drift_lon = around_lon(widened(stat_f[0]), nb_f[1], nb_f[0])
        drift_lat = around_lat(widened(stat_f[1]), nb_f[3], nb_f[2])
        wet = widened(sea_of(stat_i[1])) * sea
        lon = lon_faces(sea_lon, drift_lon)
        lat = lat_faces(sea_lat, drift_lat)
        places = []
        for field, dst in zip(lon, (oxs, pxs)):
            places += [(field, dst, 0, inside, 31), (field, dst, rows, inside, rows - 1)]
        spread(places)
        fields = list(lon) + [pltpu.roll(field, 1, 0) for field in lon]
        fields += list(lat) + [pltpu.roll(field, 1, 1) for field in lat]
        fields += [widened(stat_f[2]) * wet, widened(stat_f[3]) * wet, sea]
        for k, j in enumerate((0, cols - 1)):
            for m, field in enumerate(fields):
                dc[k, m] = jnp.broadcast_to(field[0:rows, j : j + 1], (rows, LANES))

    def width_of(t):
        return LANES if t < mains else tail

    def at(main, last, r, t, line):
        if t < mains:
            return main[r, t, pl.ds(line, 8), :]
        return last[r, pl.ds(line, 8), :]

    def put(main, last, r, t, line, value):
        if t < mains:
            main[r, t, pl.ds(line, 8), :] = value
        else:
            last[r, pl.ds(line, 8), :] = value

    def table(k, t):
        return tab[k * pieces + t, :, pl.ds(0, width_of(t))]

    def faces(i, jt, t):
        cut = (slice(None), slice(0, width_of(t)))
        line = PAD + 8 * jt
        cos_speed, sin_speed = table(0, t), table(1, t)
        spot = pl.ds(8 * jt, 8)
        a_e = oxs[i + 1, spot, :][cut] * cos_speed + pxs[i + 1, spot, :][cut]
        a_w = oxs[i, spot, :][cut] * cos_speed + pxs[i, spot, :][cut]
        a_n = oys[i, pl.ds(line, 8), :][cut] * sin_speed + pys[i, pl.ds(line, 8), :][cut]
        a_s = oys[i, pl.ds(line - 1, 8), :][cut] * sin_speed + pys[i, pl.ds(line - 1, 8), :][cut]
        return a_e, a_w, a_n, a_s

    scale = 1.0 / bins

    def lon_flux(i, jt, t):
        cut = (slice(None), slice(0, width_of(t)))
        spot = pl.ds(8 * jt, 8)
        line = PAD + 8 * jt
        pace = oxs[i + 1, spot, :][cut] * table(0, t) + pxs[i + 1, spot, :][cut]
        here, e = at(sp_main, sp_tail, i + 1, t, line), at(sp_main, sp_tail, i + 2, t, line)
        if isinstance(i, int) and i < 0:
            return pace * jnp.where(pace > 0.0, here, e)
        return pace * jnp.where(pace < 0.0, e, here)

    def tally(i, jt, parts):
        whole = parts[0]
        for more in parts[1:mains]:
            whole = whole + more
        part[i, jt] = whole
        part[i, jt, :, pl.ds(0, tail)] = whole[:, :tail] + parts[mains]

    def prime(i, jts):
        for jt in jts:
            for t in range(pieces):
                fx[jt, t, :, pl.ds(0, width_of(t))] = lon_flux(i - 1, jt, t)

    def advect(i, jts):
        for jt in jts:
            parts = []
            spot = pl.ds(PAD + 8 * jt, 8)
            under = pl.ds(PAD + 8 * jt - 1, 8)
            for t in range(pieces):
                width = width_of(t)
                cut = (slice(None), slice(0, width))
                sin_speed = table(1, t)
                a_n = oys[i, spot, :][cut] * sin_speed + pys[i, spot, :][cut]
                a_s = oys[i, under, :][cut] * sin_speed + pys[i, under, :][cut]
                line = PAD + 8 * jt
                here = at(sp_main, sp_tail, i + 1, t, line)
                n = at(sp_main, sp_tail, i + 1, t, line + 1)
                s = at(sp_main, sp_tail, i + 1, t, line - 1)
                f_w = fx[jt, t, :, pl.ds(0, width)]
                f_e = lon_flux(i, jt, t)
                fx[jt, t, :, pl.ds(0, width)] = f_e
                lat = a_n * jnp.where(a_n < 0.0, n, here) - a_s * jnp.where(a_s > 0.0, s, here)
                moved = here - (f_e - f_w) - lat
                adv[i, jt, t, :, pl.ds(0, width)] = moved
                parts.append(moved)
            tally(i, jt, parts)

    def gather(low, count, jt, tall):
        block = (pl.ds(low, count), pl.ds(jt, tall))
        level[block] = jnp.broadcast_to(
            jnp.sum(part[block], axis=3, keepdims=True) * scale, (count, tall, 8, LANES)
        )

    def weigh(i, jts):
        for jt in jts:
            parts = []
            spot = pl.ds(8 * jt, 8)
            energy = level[i, jt]
            for t in range(pieces):
                width = width_of(t)
                cut = (slice(None), slice(0, width))
                moved = adv[i, jt, t, :, pl.ds(0, width)]
                blow = wxs[i, spot, :][cut] * table(2, t) + wys[i, spot, :][cut] * table(3, t)
                gain = jnp.maximum(blow, 0.0) + seas[i, spot, :][cut]
                loss = table(4, t) * moved
                damp = 1.0 + energy[cut] * loss
                square = damp * damp
                inverse = pl.reciprocal(square, approx=True)
                inverse = inverse * (2.0 - square * inverse)
                weighted = inc[i, spot, pl.ds(t * LANES, width)] * gain * inverse
                put(ss_main, ss_tail, i + 1, t, PAD + 8 * jt, weighted)
                parts.append(weighted * loss * moved)
            tally(i, jt, parts)

    def settle(i, jts):
        for jt in jts:
            line = PAD + 8 * jt
            pull = level[i, jt]
            for t in range(pieces):
                value = at(ss_main, ss_tail, i + 1, t, line) - pull[:, : width_of(t)]
                put(ss_main, ss_tail, i + 1, t, line, value)

    def source(low, count, jts, before_weigh=None):
        jts = list(jts)
        prime(low, jts)
        spans = [(jts[0], len(jts))] if jts[-1] - jts[0] == len(jts) - 1 else [(jt, 1) for jt in jts]
        for step in (advect, weigh, settle):
            if step is weigh and before_weigh is not None:
                before_weigh()
            if count == 1:
                step(low, jts)
            else:
                looped(low, low + count, lambda i: step(i, jts))
            if step is not settle:
                for jt, tall in spans:
                    gather(low, count, jt, tall)

    row_at = lax.broadcasted_iota(jnp.int32, (rows, LANES), 0)

    def line(main, last, r, t, place):
        if t < mains:
            return main.at[r, t, pl.ds(place, 1), :]
        return last.at[r, pl.ds(place, 1), :]

    def lanes_of(t):
        return pl.ds(t * LANES, width_of(t))

    def lane_sum(parts):
        whole = parts[0]
        for more in parts[1:mains]:
            whole = whole + more
        return jnp.sum(whole, axis=1, keepdims=True) + jnp.sum(parts[mains], axis=1, keepdims=True)

    def wide_table(k, t):
        return jnp.broadcast_to(tab[k * pieces + t, pl.ds(0, 1), pl.ds(0, width_of(t))], (rows, width_of(t)))

    def edge_columns():
        ends = (0, 1)
        places = (PAD, PAD + cols - 1)
        sums = [[], []]
        for k in ends:
            here_at, n_at, s_at = ((1, 2, 0), (4, 5, 3))[k]
            for t in range(pieces):
                width = width_of(t)
                coef = [dc[k, m][:, :width] for m in range(8)]
                cos_speed, sin_speed = wide_table(0, t), wide_table(1, t)
                here = col[here_at, :, lanes_of(t)]
                n, s = col[n_at, :, lanes_of(t)], col[s_at, :, lanes_of(t)]
                e_end = line(sp_main, sp_tail, rows + 1, t, places[k])[...]
                w_end = line(sp_main, sp_tail, 0, t, places[k])[...]
                at_row = row_at[:, :width]
                e = jnp.where(at_row == rows - 1, e_end, pltpu.roll(here, rows - 1, 0))
                w = jnp.where(at_row == 0, w_end, pltpu.roll(here, 1, 0))
                a_e = coef[0] * cos_speed + coef[1]
                a_w = coef[2] * cos_speed + coef[3]
                a_n = coef[4] * sin_speed + coef[5]
                a_s = coef[6] * sin_speed + coef[7]
                lon = a_e * jnp.where(a_e < 0.0, e, here) - a_w * jnp.where(a_w > 0.0, w, here)
                lat = a_n * jnp.where(a_n < 0.0, n, here) - a_s * jnp.where(a_s > 0.0, s, here)
                moved = here - lon - lat
                sc[1 + k, :, lanes_of(t)] = moved
                sums[k].append(moved)
        energies = [lane_sum(sums[k]) * scale for k in ends]
        pulls = [[], []]
        for k in ends:
            energy = jnp.broadcast_to(energies[k], (rows, LANES))
            for t in range(pieces):
                width = width_of(t)
                wind_x, wind_y, open_sea = [dc[k, m][:, :width] for m in range(8, 11)]
                moved = sc[1 + k, :, lanes_of(t)]
                blow = wind_x * wide_table(2, t) + wind_y * wide_table(3, t)
                gain = jnp.maximum(blow, 0.0) + open_sea
                loss = wide_table(4, t) * moved
                damp = 1.0 + energy[:, :width] * loss
                square = damp * damp
                inverse = pl.reciprocal(square, approx=True)
                inverse = inverse * (2.0 - square * inverse)
                weighted = ci[k, :, lanes_of(t)] * gain * inverse
                sc[1 + k, :, lanes_of(t)] = weighted
                pulls[k].append(weighted * loss * moved)
        ends_pull = [lane_sum(pulls[k]) * scale for k in ends]
        for k in ends:
            pull = jnp.broadcast_to(ends_pull[k], (rows, LANES))
            for t in range(pieces):
                sc[1 + k, :, lanes_of(t)] = sc[1 + k, :, lanes_of(t)] - pull[:, : width_of(t)]

    def insert_columns(which):
        for i in which:
            for k, place in enumerate((PAD, PAD + cols - 1)):
                for t in range(pieces):
                    target = line(ss_main, ss_tail, i + 1, t, place)
                    target[...] = sc[1 + k, pl.ds(i, 1), lanes_of(t)]

    def transport(cells, skip_e=False, skip_w=False):
        for i, jt in cells:
            for t in range(pieces):
                a_e, a_w, a_n, a_s = faces(i, jt, t)
                place = PAD + 8 * jt
                here = at(ss_main, ss_tail, i + 1, t, place)
                n = at(ss_main, ss_tail, i + 1, t, place + 1)
                s = at(ss_main, ss_tail, i + 1, t, place - 1)
                total = here
                if not skip_e:
                    e = at(ss_main, ss_tail, i + 2, t, place)
                    total = total + jnp.maximum(a_e, 0.0) * (e - here)
                if not skip_w:
                    w = at(ss_main, ss_tail, i, t, place)
                    total = total + jnp.minimum(a_w, 0.0) * (here - w)
                if jt == tiles - 1:
                    total = total + jnp.where(a_n > 0.0, a_n * (n - here), 0.0)
                else:
                    total = total + jnp.maximum(a_n, 0.0) * (n - here)
                if jt == 0:
                    total = total + jnp.where(a_s < 0.0, a_s * (here - s), 0.0)
                else:
                    total = total + jnp.minimum(a_s, 0.0) * (here - s)
                out[i, pl.ds(8 * jt, 8), lanes_of(t)] = total

    def finish_row(i):
        for jt in range(tiles):
            spot = pl.ds(8 * jt, 8)
            for t in range(pieces):
                if t in (idle_two["east"] if i == 0 else idle_two["west"]):
                    continue
                cut = (slice(None), slice(0, width_of(t)))
                here = at(ss_main, ss_tail, i + 1, t, PAD + 8 * jt)
                if i == 0:
                    a_w = oxs[0, spot, :][cut] * table(0, t) + pxs[0, spot, :][cut]
                    term = jnp.minimum(a_w, 0.0) * (here - at(ss_main, ss_tail, 0, t, PAD + 8 * jt))
                else:
                    a_e = oxs[rows, spot, :][cut] * table(0, t) + pxs[rows, spot, :][cut]
                    far = at(ss_main, ss_tail, rows + 1, t, PAD + 8 * jt)
                    term = jnp.maximum(a_e, 0.0) * (far - here)
                out[i, spot, lanes_of(t)] = out[i, spot, lanes_of(t)] + term

    def finish_column(k):
        for t in range(pieces):
            width = width_of(t)
            here = sc[1 + k, :, lanes_of(t)]
            if k == 0:
                a_s = dc[0, 6][:, :width] * wide_table(1, t) + dc[0, 7][:, :width]
                term = jnp.where(a_s < 0.0, a_s * (here - sc[0, :, lanes_of(t)]), 0.0)
            else:
                a_n = dc[1, 4][:, :width] * wide_table(1, t) + dc[1, 5][:, :width]
                term = jnp.where(a_n > 0.0, a_n * (sc[3, :, lanes_of(t)] - here), 0.0)
            ci[k, :, lanes_of(t)] = term
        place = pl.ds(0 if k == 0 else cols - 1, 1)
        for i in range(rows):
            for t in range(pieces):
                term = ci[k, pl.ds(i, 1), lanes_of(t)]
                out[i, place, lanes_of(t)] = out[i, place, lanes_of(t)] + term

    def looped(low, high, run):
        def step(i, carry):
            run(i)
            return carry

        lax.fori_loop(low, high, step, 0)

    everywhere = range(tiles)
    early = gy == ny // 2
    late = gy != ny // 2
    from_fold = lax.rem(gy + ny // 2, ny)
    beside = jnp.logical_or(from_fold < 2, from_fold >= ny - 1)
    beside = jnp.logical_or(beside, jnp.logical_or(gy == 0, gy == ny - 1))
    away = jnp.logical_not(beside)
    first_part = (rows - 2) * 5 // 11

    def first_source():
        prepare()
        for copy in bulk:
            copy.wait()
        source(1, first_part, everywhere, inc_load.wait)

    def second_source():
        source(1 + first_part, rows - 2 - first_part, everywhere)

    for copy in small[:3] + last_row + first_row + col_loads[:2]:
        copy.wait()
    pl.when(early)(first_source)
    peers = 2 + lax.div(gy + ny - 1, ny) + lax.div(2 * ny - 2 - gy, ny)
    pl.semaphore_wait(barrier, peers)
    for side in sides:
        start(stat_copies, side)
    for side in ("north", "south", "east", "west"):
        start(one, side)
    pl.when(late)(first_source)
    pl.when(beside)(second_source)
    for copy in col_loads[2:] + ci_loads:
        copy.wait()
    for side in sides:
        wait_recv(stat_copies, side)
    prepare_edges()
    for side in sides:
        wait_recv(one, side)
    edge_columns()
    start(two, "north")
    start(two, "south")
    source(rows - 1, 1, everywhere)
    source(0, 1, everywhere)
    insert_columns((0, rows - 1))
    start(two, "east")
    start(two, "west")
    pl.when(away)(second_source)
    insert_columns(range(1, rows - 1))
    looped(1, rows - 1, lambda i: transport([(i, jt) for jt in everywhere]))
    transport([(0, jt) for jt in everywhere], skip_w=True)
    transport([(rows - 1, jt) for jt in everywhere], skip_e=True)
    for side in ("west", "east"):
        wait_recv(two, side)
    finish_row(rows - 1)
    finish_row(0)
    wait_recv(two, "south")
    finish_column(1)
    wait_recv(two, "north")
    finish_column(0)
    for group in (stat_copies, one, two):
        for side in sides:
            wait_send(group, side)


def body(
    spectrum,
    adjoint_in,
    current_x,
    current_y,
    wind_x,
    wind_y,
    land_mask,
    ice_mask,
    group_speed,
    growth_rate,
    dissipation,
):
    rows, cols, bins = spectrum.shape
    freqs = group_speed.shape[0]
    wave = np.zeros((8, -(-bins // LANES) * LANES), np.float32)
    wave[0, :bins], wave[1, :bins] = directions(bins)
    mains = bins // LANES
    tail = bins - mains * LANES
    tall = cols + 2 * PAD
    f32 = jnp.float32
    any_space = pl.BlockSpec(memory_space=pl.ANY)
    return pl.pallas_call(
        kernel,
        out_shape=pltpu.VMEM((rows, cols, bins), f32),
        in_specs=[any_space] * 12,
        out_specs=pl.BlockSpec(memory_space=pltpu.VMEM),
        scratch_shapes=[
            pltpu.VMEM((rows + 2, mains, tall, LANES), f32),
            pltpu.VMEM((rows + 2, tall, tail), f32),
            pltpu.VMEM((rows + 2, mains, tall, LANES), f32),
            pltpu.VMEM((rows + 2, tall, tail), f32),
            pltpu.VMEM((rows, cols, bins), f32),
            pltpu.VMEM((rows, cols // 8, mains + 1, 8, LANES), f32),
            pltpu.VMEM((rows + 1, cols, LANES), f32),
            pltpu.VMEM((rows + 1, cols, LANES), f32),
            pltpu.VMEM((rows, tall, LANES), f32),
            pltpu.VMEM((rows, tall, LANES), f32),
            pltpu.VMEM((rows, cols, LANES), f32),
            pltpu.VMEM((rows, cols, LANES), f32),
            pltpu.VMEM((rows, cols, LANES), f32),
            pltpu.VMEM((cols // 8, mains + 1, 8, LANES), f32),
            pltpu.VMEM((rows, cols // 8, 8, LANES), f32),
            pltpu.VMEM((rows, cols // 8, 8, LANES), f32),
            pltpu.VMEM((6, rows, bins), f32),
            pltpu.VMEM((2, rows, bins), f32),
            pltpu.VMEM((4, rows, bins), f32),
            pltpu.VMEM((2, 11, rows, LANES), f32),
            pltpu.VMEM((3, 1, freqs), f32),
            pltpu.VMEM(wave.shape, f32),
            pltpu.VMEM((8, LANES), f32),
            pltpu.VMEM((5 * (mains + 1), 8, LANES), f32),
            pltpu.VMEM((4, rows, cols), f32),
            pltpu.VMEM((2, rows, cols), jnp.int32),
            pltpu.VMEM((4, rows, cols), f32),
            pltpu.VMEM((4, rows, cols), jnp.int32),
            pltpu.VMEM((32, LANES), f32),
            pltpu.SemaphoreType.DMA((3 * (mains + 1) + 17,)),
            pltpu.SemaphoreType.DMA((24,)),
            pltpu.SemaphoreType.DMA((24,)),
        ],
        compiler_params=pltpu.CompilerParams(
            collective_id=0, has_side_effects=True, vmem_limit_bytes=50 * 1024 * 1024
        ),
    )(
        spectrum,
        adjoint_in,
        current_x,
        current_y,
        wind_x,
        wind_y,
        land_mask,
        ice_mask,
        group_speed.reshape(1, freqs),
        growth_rate.reshape(1, freqs),
        dissipation.reshape(1, freqs),
        jnp.asarray(wave),
    )


def solution(mesh):
    cells = P("gx", "gy", None)
    placed = (cells, cells) + (P("gx", "gy"),) * 6 + (P(),) * 3
    return jax.shard_map(body, mesh=mesh, in_specs=placed, out_specs=cells, check_vma=False)
```

```python
import math

import jax
import jax.numpy as jnp
import numpy as np
from jax import lax
from jax.experimental import pallas as pl
from jax.experimental.pallas import tpu as pltpu
from jax.sharding import PartitionSpec as P

DIRS = 36
LANES = 128
LEAST_SPEED = 0.1
MOST_CURRENT = 0.08
PAD = 8
MESH = pl.DeviceIdType.MESH


def directions(bins):
    angles = np.float32(2.0 * math.pi / DIRS) * (np.arange(DIRS, dtype=np.float32) + np.float32(0.5))
    per_dir = bins // DIRS
    return np.repeat(np.cos(angles), per_dir), np.repeat(np.sin(angles), per_dir)


def one_way(heading):
    sure = 1.001 * MOST_CURRENT / LEAST_SPEED
    starts = range(0, heading.size, LANES)
    forward = [t for t, b in enumerate(starts) if np.all(heading[b : b + LANES] > sure)]
    backward = [t for t, b in enumerate(starts) if np.all(heading[b : b + LANES] < -sure)]
    return forward, backward


def kernel(
    spec_hbm,
    adj_hbm,
    cx_hbm,
    cy_hbm,
    wx_hbm,
    wy_hbm,
    land_hbm,
    ice_hbm,
    speed_hbm,
    growth_hbm,
    loss_hbm,
    wave_hbm,
    out,
    sp_main,
    sp_tail,
    ss_main,
    ss_tail,
    inc,
    adv,
    oxs,
    pxs,
    oys,
    pys,
    wxs,
    wys,
    seas,
    fx,
    part,
    level,
    col,
    ci,
    sc,
    dc,
    par_in,
    wave,
    par,
    tab,
    stat_f,
    stat_i,
    nb_f,
    nb_i,
    ext,
    load_sem,
    send_sem,
    recv_sem,
):
    rows, cols, bins = spec_hbm.shape
    mains = bins // LANES
    tail = bins - mains * LANES
    tiles = cols // 8
    pieces = mains + 1
    gx = lax.axis_index("gx")
    gy = lax.axis_index("gy")
    nx = lax.axis_size("gx")
    ny = lax.axis_size("gy")
    east = lax.rem(gx + 1, nx)
    west = lax.rem(gx + nx - 1, nx)
    has_north = gy < ny - 1
    has_south = gy > 0
    body = pl.ds(PAD, cols)

    barrier = pltpu.get_barrier_semaphore()
    for target in (east, west):
        pl.semaphore_signal(barrier, inc=1, device_id={"gx": target}, device_id_type=MESH)

    @pl.when(has_north)
    def _():
        pl.semaphore_signal(barrier, inc=1, device_id={"gy": gy + 1}, device_id_type=MESH)

    @pl.when(has_south)
    def _():
        pl.semaphore_signal(barrier, inc=1, device_id={"gy": gy - 1}, device_id_type=MESH)

    def local(src, dst, k):
        return pltpu.make_async_copy(src, dst, load_sem.at[k])

    def loads_of(low, count, base):
        copies = []
        for t in range(pieces):
            src_lanes = pl.ds(t * LANES, LANES if t < mains else tail)
            src = spec_hbm.at[pl.ds(low, count), :, src_lanes]
            if t < mains:
                dst = sp_main.at[pl.ds(low + 1, count), t, body, :]
            else:
                dst = sp_tail.at[pl.ds(low + 1, count), body, :]
            copies.append(local(src, dst, base + t))
        return copies

    first_row = loads_of(0, 1, 0)
    last_row = loads_of(rows - 1, 1, pieces)
    bulk = loads_of(1, rows - 2, 2 * pieces)
    base = 3 * pieces
    small = [
        local(land_hbm, stat_i.at[0], base),
        local(cx_hbm, stat_f.at[0], base + 1),
        local(cy_hbm, stat_f.at[1], base + 2),
        local(wx_hbm, stat_f.at[2], base + 3),
        local(wy_hbm, stat_f.at[3], base + 4),
        local(ice_hbm, stat_i.at[1], base + 5),
        local(speed_hbm, par_in.at[0], base + 6),
        local(growth_hbm, par_in.at[1], base + 7),
        local(loss_hbm, par_in.at[2], base + 8),
        local(wave_hbm, wave, base + 9),
    ]
    inc_load = local(adj_hbm, inc, base + 10)
    col_loads = [
        local(spec_hbm.at[:, j, :], col.at[k], base + 10 + k)
        for k, j in ((1, 0), (4, cols - 1), (2, 1), (3, cols - 2))
    ]
    ci_loads = [
        local(adj_hbm.at[:, j, :], ci.at[k], base + 15 + k) for k, j in ((0, 0), (1, cols - 1))
    ]
    for copy in small + last_row + first_row + col_loads + bulk + ci_loads + [inc_load]:
        copy.start()

    def remote(src, dst, k, device):
        return pltpu.make_async_remote_copy(
            src_ref=src,
            dst_ref=dst,
            send_sem=send_sem.at[k],
            recv_sem=recv_sem.at[k],
            device_id=device,
            device_id_type=MESH,
        )

    to_east, to_west = {"gx": east}, {"gx": west}
    to_north, to_south = {"gy": gy + 1}, {"gy": gy - 1}

    used = iter(range(24))

    def runs(skip):
        spans, low = [], 0
        for t in sorted(skip) + [pieces]:
            if t > low:
                spans.append((low, t))
            low = t + 1
        return spans

    def edge(main, last, lines, side, skip):
        copies = []
        for low, high in runs(skip):
            if side in ("north", "south"):
                lanes = pl.ds(low * LANES, min(high * LANES, bins) - low * LANES)
                top = lines.shape[0] - 1
                src, dst, device = (top - 1, 0, to_north) if side == "north" else (1, top, to_south)
                copies.append(
                    remote(lines.at[src, :, lanes], lines.at[dst, :, lanes], next(used), device)
                )
                continue
            src, dst, device = (rows, 0, to_east) if side == "east" else (1, rows + 1, to_west)
            whole = pl.ds(low, min(high, mains) - low)
            copies.append(
                remote(main.at[src, whole, body, :], main.at[dst, whole, body, :], next(used), device)
            )
            if high == pieces:
                copies.append(
                    remote(last.at[src, body, :], last.at[dst, body, :], next(used), device)
                )
        return copies

    sides = ("east", "west", "north", "south")
    stat_copies = {}
    for s, (side, device, field) in enumerate(
        (("east", to_east, 0), ("west", to_west, 0), ("north", to_north, 1), ("south", to_south, 1))
    ):
        stat_copies[side] = [
            remote(stat_i.at[0], nb_i.at[s], next(used), device),
            remote(stat_f.at[field], nb_f.at[s], next(used), device),
        ]
    cosine, sine = directions(bins)
    (eastward, westward), (northward, southward) = one_way(cosine), one_way(sine)
    idle_one = {"east": westward, "west": eastward, "north": southward, "south": northward}
    idle_two = {"east": eastward, "west": westward, "north": northward, "south": southward}
    one = {side: edge(sp_main, sp_tail, col, side, idle_one[side]) for side in sides}
    two = {side: edge(ss_main, ss_tail, sc, side, idle_two[side]) for side in sides}

    sends_ok = {"east": None, "west": None, "north": has_north, "south": has_south}
    recvs_ok = {"east": None, "west": None, "north": has_south, "south": has_north}

    def guarded(condition, run):
        if condition is None:
            run()
        else:
            pl.when(condition)(run)

    def start(group, side):
        guarded(sends_ok[side], lambda: [copy.start() for copy in group[side]] and None)

    def wait_recv(group, side):
        guarded(recvs_ok[side], lambda: [copy.wait_recv() for copy in group[side]] and None)

    def wait_send(group, side):
        guarded(sends_ok[side], lambda: [copy.wait_send() for copy in group[side]] and None)

    lane = lax.broadcasted_iota(jnp.int32, (32, LANES), 1)
    row = lax.broadcasted_iota(jnp.int32, (32, LANES), 0)

    def widened(values):
        ext[...] = jnp.zeros((32, LANES), jnp.float32)
        ext[pl.ds(0, rows), pl.ds(0, cols)] = values
        return ext[...]

    def sea_of(mask):
        return (1 - mask).astype(jnp.float32)

    def around_lon(mine, from_east, from_west):
        up = pltpu.roll(widened(from_east), rows, 0)
        down = pltpu.roll(widened(from_west), 8, 0)
        return jnp.where(row == rows, up, jnp.where(row == 31, down, mine))

    def around_lat(mine, from_north, from_south):
        up = pltpu.roll(widened(from_north), cols, 1)
        down = pltpu.roll(widened(from_south), LANES - cols, 1)
        up = jnp.where(has_north, up, 0.0)
        down = jnp.where(has_south, down, 0.0)
        return jnp.where(lane == cols, up, jnp.where(lane == LANES - 1, down, mine))

    def spread(places):
        turned = {}
        for field, dst, spot, column, r in places:
            if id(field) not in turned:
                turned[id(field)] = jnp.transpose(field)
        for field, dst, spot, column, r in sorted(places, key=lambda place: place[4]):
            count = column.stop - column.start
            dst[spot] = jnp.broadcast_to(turned[id(field)][column, r : r + 1], (count, LANES))

    inside = slice(0, cols)
    inside_at = pl.ds(PAD, cols)

    def lon_faces(sea_lon, drift_lon):
        opened = sea_lon * pltpu.roll(sea_lon, 31, 0)
        return opened, opened * (0.5 * (drift_lon + pltpu.roll(drift_lon, 31, 0)))

    def lat_faces(sea_lat, drift_lat):
        opened = sea_lat * pltpu.roll(sea_lat, LANES - 1, 1)
        return opened, opened * (0.5 * (drift_lat + pltpu.roll(drift_lat, LANES - 1, 1)))

    def prepare():
        for copy in small[3:]:
            copy.wait()
        par[...] = jnp.zeros((8, LANES), jnp.float32)
        freqs = speed_hbm.shape[1]
        for k in range(3):
            par[pl.ds(k, 1), pl.ds(0, freqs)] = par_in[k]
        per_freq = par[...]
        bin_lane = lax.broadcasted_iota(jnp.int32, (8, LANES), 1)
        for t in range(pieces):
            freq = lax.rem(bin_lane + t * LANES, freqs)
            picked = jnp.take_along_axis(per_freq, freq, axis=1)
            full = (8, LANES)
            speed = jnp.broadcast_to(picked[0:1], full)
            growth = jnp.broadcast_to(picked[1:2], full)
            cosine = jnp.broadcast_to(wave[pl.ds(0, 1), pl.ds(t * LANES, LANES)], full)
            sine = jnp.broadcast_to(wave[pl.ds(1, 1), pl.ds(t * LANES, LANES)], full)
            tab[t] = speed * cosine
            tab[pieces + t] = speed * sine
            tab[2 * pieces + t] = growth * cosine
            tab[3 * pieces + t] = growth * sine
            tab[4 * pieces + t] = jnp.broadcast_to(picked[2:3], full)
        sea = widened(sea_of(stat_i[0]))
        wet = widened(sea_of(stat_i[1])) * sea
        every = range(rows)
        lon = lon_faces(sea, widened(stat_f[0]))
        lat = lat_faces(sea, widened(stat_f[1]))
        breeze = [widened(stat_f[2]) * wet, widened(stat_f[3]) * wet]
        places = []
        for r in every:
            places += [(field, dst, r, inside, r) for field, dst in zip(breeze + [sea], (wxs, wys, seas))]
            places += [(field, dst, (r, inside_at), inside, r) for field, dst in zip(lat, (oys, pys))]
            if r < rows - 1:
                places += [(field, dst, r + 1, inside, r) for field, dst in zip(lon, (oxs, pxs))]
        spread(places)
        for dst in (oys, pys):
            for r in every:
                dst[r, pl.ds(0, PAD), :] = jnp.zeros((PAD, LANES), jnp.float32)

    def prepare_edges():
        sea = widened(sea_of(stat_i[0]))
        sea_lon = around_lon(sea, sea_of(nb_i[1]), sea_of(nb_i[0]))
        sea_lat = around_lat(sea, sea_of(nb_i[3]), sea_of(nb_i[2]))
        drift_lon = around_lon(widened(stat_f[0]), nb_f[1], nb_f[0])
        drift_lat = around_lat(widened(stat_f[1]), nb_f[3], nb_f[2])
        wet = widened(sea_of(stat_i[1])) * sea
        lon = lon_faces(sea_lon, drift_lon)
        lat = lat_faces(sea_lat, drift_lat)
        places = []
        for field, dst in zip(lon, (oxs, pxs)):
            places += [(field, dst, 0, inside, 31), (field, dst, rows, inside, rows - 1)]
        spread(places)
        fields = list(lon) + [pltpu.roll(field, 1, 0) for field in lon]
        fields += list(lat) + [pltpu.roll(field, 1, 1) for field in lat]
        fields += [widened(stat_f[2]) * wet, widened(stat_f[3]) * wet, sea]
        for k, j in enumerate((0, cols - 1)):
            for m, field in enumerate(fields):
                dc[k, m] = jnp.broadcast_to(field[0:rows, j : j + 1], (rows, LANES))

    def width_of(t):
        return LANES if t < mains else tail

    def at(main, last, r, t, line):
        if t < mains:
            return main[r, t, pl.ds(line, 8), :]
        return last[r, pl.ds(line, 8), :]

    def put(main, last, r, t, line, value):
        if t < mains:
            main[r, t, pl.ds(line, 8), :] = value
        else:
            last[r, pl.ds(line, 8), :] = value

    def table(k, t):
        return tab[k * pieces + t, :, pl.ds(0, width_of(t))]

    def faces(i, jt, t):
        cut = (slice(None), slice(0, width_of(t)))
        line = PAD + 8 * jt
        cos_speed, sin_speed = table(0, t), table(1, t)
        spot = pl.ds(8 * jt, 8)
        a_e = oxs[i + 1, spot, :][cut] * cos_speed + pxs[i + 1, spot, :][cut]
        a_w = oxs[i, spot, :][cut] * cos_speed + pxs[i, spot, :][cut]
        a_n = oys[i, pl.ds(line, 8), :][cut] * sin_speed + pys[i, pl.ds(line, 8), :][cut]
        a_s = oys[i, pl.ds(line - 1, 8), :][cut] * sin_speed + pys[i, pl.ds(line - 1, 8), :][cut]
        return a_e, a_w, a_n, a_s

    scale = 1.0 / bins

    def lon_flux(i, jt, t, from_west=False):
        cut = (slice(None), slice(0, width_of(t)))
        spot = pl.ds(8 * jt, 8)
        line = PAD + 8 * jt
        pace = oxs[i + 1, spot, :][cut] * table(0, t) + pxs[i + 1, spot, :][cut]
        here, e = at(sp_main, sp_tail, i + 1, t, line), at(sp_main, sp_tail, i + 2, t, line)
        if from_west:
            return jnp.where(pace > 0.0, pace * here, jnp.where(pace < 0.0, pace * e, 0.0))
        return pace * jnp.where(pace < 0.0, e, here)

    def tally(i, jt, parts):
        whole = parts[0]
        for more in parts[1:mains]:
            whole = whole + more
        part[i, jt] = whole
        part[i, jt, :, pl.ds(0, tail)] = whole[:, :tail] + parts[mains]

    def prime(i, jts):
        for jt in jts:
            for t in range(pieces):
                fx[jt, t, :, pl.ds(0, width_of(t))] = lon_flux(i - 1, jt, t, True)

    def advect(i, jts):
        for jt in jts:
            parts = []
            spot = pl.ds(PAD + 8 * jt, 8)
            under = pl.ds(PAD + 8 * jt - 1, 8)
            for t in range(pieces):
                width = width_of(t)
                cut = (slice(None), slice(0, width))
                sin_speed = table(1, t)
                a_n = oys[i, spot, :][cut] * sin_speed + pys[i, spot, :][cut]
                a_s = oys[i, under, :][cut] * sin_speed + pys[i, under, :][cut]
                line = PAD + 8 * jt
                here = at(sp_main, sp_tail, i + 1, t, line)
                n = at(sp_main, sp_tail, i + 1, t, line + 1)
                s = at(sp_main, sp_tail, i + 1, t, line - 1)
                f_w = fx[jt, t, :, pl.ds(0, width)]
                f_e = lon_flux(i, jt, t)
                fx[jt, t, :, pl.ds(0, width)] = f_e
                lat = a_n * jnp.where(a_n < 0.0, n, here) - a_s * jnp.where(a_s > 0.0, s, here)
                moved = here - (f_e - f_w) - lat
                adv[i, jt, t, :, pl.ds(0, width)] = moved
                parts.append(moved)
            tally(i, jt, parts)

    def gather(low, count, jt, tall):
        block = (pl.ds(low, count), pl.ds(jt, tall))
        level[block] = jnp.broadcast_to(
            jnp.sum(part[block], axis=3, keepdims=True) * scale, (count, tall, 8, LANES)
        )

    def weigh(i, jts):
        for jt in jts:
            parts = []
            spot = pl.ds(8 * jt, 8)
            energy = level[i, jt]
            for t in range(pieces):
                width = width_of(t)
                cut = (slice(None), slice(0, width))
                moved = adv[i, jt, t, :, pl.ds(0, width)]
                blow = wxs[i, spot, :][cut] * table(2, t) + wys[i, spot, :][cut] * table(3, t)
                gain = jnp.maximum(blow, 0.0) + seas[i, spot, :][cut]
                loss = table(4, t) * moved
                damp = 1.0 + energy[cut] * loss
                square = damp * damp
                inverse = pl.reciprocal(square, approx=True)
                inverse = inverse * (2.0 - square * inverse)
                weighted = inc[i, spot, pl.ds(t * LANES, width)] * gain * inverse
                put(ss_main, ss_tail, i + 1, t, PAD + 8 * jt, weighted)
                parts.append(weighted * loss * moved)
            tally(i, jt, parts)

    def settle(i, jts):
        for jt in jts:
            line = PAD + 8 * jt
            pull = level[i, jt]
            for t in range(pieces):
                value = at(ss_main, ss_tail, i + 1, t, line) - pull[:, : width_of(t)]
                put(ss_main, ss_tail, i + 1, t, line, value)

    def source(low, count, jts, before_weigh=None):
        jts = list(jts)
        prime(low, jts)
        spans = [(jts[0], len(jts))] if jts[-1] - jts[0] == len(jts) - 1 else [(jt, 1) for jt in jts]
        for step in (advect, weigh, settle):
            if step is weigh and before_weigh is not None:
                before_weigh()
            if count == 1:
                step(low, jts)
            else:
                looped(low, low + count, lambda i: step(i, jts))
            if step is not settle:
                for jt, tall in spans:
                    gather(low, count, jt, tall)

    row_at = lax.broadcasted_iota(jnp.int32, (rows, LANES), 0)

    def line(main, last, r, t, place):
        if t < mains:
            return main.at[r, t, pl.ds(place, 1), :]
        return last.at[r, pl.ds(place, 1), :]

    def lanes_of(t):
        return pl.ds(t * LANES, width_of(t))

    def lane_sum(parts):
        whole = parts[0]
        for more in parts[1:mains]:
            whole = whole + more
        return jnp.sum(whole, axis=1, keepdims=True) + jnp.sum(parts[mains], axis=1, keepdims=True)

    def wide_table(k, t):
        return jnp.broadcast_to(tab[k * pieces + t, pl.ds(0, 1), pl.ds(0, width_of(t))], (rows, width_of(t)))

    def edge_columns(ends):
        places = (PAD, PAD + cols - 1)
        sums = [[], []]
        for k in ends:
            here_at, n_at, s_at = ((1, 2, 0), (4, 5, 3))[k]
            for t in range(pieces):
                width = width_of(t)
                coef = [dc[k, m][:, :width] for m in range(8)]
                cos_speed, sin_speed = wide_table(0, t), wide_table(1, t)
                here = col[here_at, :, lanes_of(t)]
                n, s = col[n_at, :, lanes_of(t)], col[s_at, :, lanes_of(t)]
                e_end = line(sp_main, sp_tail, rows + 1, t, places[k])[...]
                w_end = line(sp_main, sp_tail, 0, t, places[k])[...]
                at_row = row_at[:, :width]
                e = jnp.where(at_row == rows - 1, e_end, pltpu.roll(here, rows - 1, 0))
                w = jnp.where(at_row == 0, w_end, pltpu.roll(here, 1, 0))
                a_e = coef[0] * cos_speed + coef[1]
                a_w = coef[2] * cos_speed + coef[3]
                a_n = coef[4] * sin_speed + coef[5]
                a_s = coef[6] * sin_speed + coef[7]
                lon = a_e * jnp.where(a_e < 0.0, e, here) - a_w * jnp.where(a_w > 0.0, w, here)
                lat = a_n * jnp.where(a_n < 0.0, n, here) - a_s * jnp.where(a_s > 0.0, s, here)
                moved = here - lon - lat
                sc[1 + k, :, lanes_of(t)] = moved
                sums[k].append(moved)
        energies = {k: lane_sum(sums[k]) * scale for k in ends}
        pulls = [[], []]
        for k in ends:
            energy = jnp.broadcast_to(energies[k], (rows, LANES))
            for t in range(pieces):
                width = width_of(t)
                wind_x, wind_y, open_sea = [dc[k, m][:, :width] for m in range(8, 11)]
                moved = sc[1 + k, :, lanes_of(t)]
                blow = wind_x * wide_table(2, t) + wind_y * wide_table(3, t)
                gain = jnp.maximum(blow, 0.0) + open_sea
                loss = wide_table(4, t) * moved
                damp = 1.0 + energy[:, :width] * loss
                square = damp * damp
                inverse = pl.reciprocal(square, approx=True)
                inverse = inverse * (2.0 - square * inverse)
                weighted = ci[k, :, lanes_of(t)] * gain * inverse
                sc[1 + k, :, lanes_of(t)] = weighted
                pulls[k].append(weighted * loss * moved)
        ends_pull = {k: lane_sum(pulls[k]) * scale for k in ends}
        for k in ends:
            pull = jnp.broadcast_to(ends_pull[k], (rows, LANES))
            for t in range(pieces):
                sc[1 + k, :, lanes_of(t)] = sc[1 + k, :, lanes_of(t)] - pull[:, : width_of(t)]

    def insert_columns(which):
        for i in which:
            for k, place in enumerate((PAD, PAD + cols - 1)):
                for t in range(pieces):
                    target = line(ss_main, ss_tail, i + 1, t, place)
                    target[...] = sc[1 + k, pl.ds(i, 1), lanes_of(t)]

    def transport(cells, skip_e=False, skip_w=False):
        for i, jt in cells:
            for t in range(pieces):
                a_e, a_w, a_n, a_s = faces(i, jt, t)
                place = PAD + 8 * jt
                here = at(ss_main, ss_tail, i + 1, t, place)
                n = at(ss_main, ss_tail, i + 1, t, place + 1)
                s = at(ss_main, ss_tail, i + 1, t, place - 1)
                total = here
                if not skip_e:
                    e = at(ss_main, ss_tail, i + 2, t, place)
                    total = total + jnp.maximum(a_e, 0.0) * (e - here)
                if not skip_w:
                    w = at(ss_main, ss_tail, i, t, place)
                    total = total + jnp.minimum(a_w, 0.0) * (here - w)
                if jt == tiles - 1:
                    total = total + jnp.where(a_n > 0.0, a_n * (n - here), 0.0)
                else:
                    total = total + jnp.maximum(a_n, 0.0) * (n - here)
                if jt == 0:
                    total = total + jnp.where(a_s < 0.0, a_s * (here - s), 0.0)
                else:
                    total = total + jnp.minimum(a_s, 0.0) * (here - s)
                out[i, pl.ds(8 * jt, 8), lanes_of(t)] = total

    def finish_row(i):
        for jt in range(tiles):
            spot = pl.ds(8 * jt, 8)
            for t in range(pieces):
                if t in (idle_two["east"] if i == 0 else idle_two["west"]):
                    continue
                cut = (slice(None), slice(0, width_of(t)))
                here = at(ss_main, ss_tail, i + 1, t, PAD + 8 * jt)
                if i == 0:
                    a_w = oxs[0, spot, :][cut] * table(0, t) + pxs[0, spot, :][cut]
                    term = jnp.minimum(a_w, 0.0) * (here - at(ss_main, ss_tail, 0, t, PAD + 8 * jt))
                else:
                    a_e = oxs[rows, spot, :][cut] * table(0, t) + pxs[rows, spot, :][cut]
                    far = at(ss_main, ss_tail, rows + 1, t, PAD + 8 * jt)
                    term = jnp.maximum(a_e, 0.0) * (far - here)
                out[i, spot, lanes_of(t)] = out[i, spot, lanes_of(t)] + term

    def finish_column(k):
        for t in range(pieces):
            width = width_of(t)
            here = sc[1 + k, :, lanes_of(t)]
            if k == 0:
                a_s = dc[0, 6][:, :width] * wide_table(1, t) + dc[0, 7][:, :width]
                term = jnp.where(a_s < 0.0, a_s * (here - sc[0, :, lanes_of(t)]), 0.0)
            else:
                a_n = dc[1, 4][:, :width] * wide_table(1, t) + dc[1, 5][:, :width]
                term = jnp.where(a_n > 0.0, a_n * (sc[3, :, lanes_of(t)] - here), 0.0)
            ci[k, :, lanes_of(t)] = term
        place = pl.ds(0 if k == 0 else cols - 1, 1)
        for i in range(rows):
            for t in range(pieces):
                term = ci[k, pl.ds(i, 1), lanes_of(t)]
                out[i, place, lanes_of(t)] = out[i, place, lanes_of(t)] + term

    def looped(low, high, run):
        def step(i, carry):
            run(i)
            return carry

        lax.fori_loop(low, high, step, 0)

    everywhere = range(tiles)
    early = gy == ny // 2
    late = gy != ny // 2
    first_part = (rows - 2) * 5 // 11

    def first_source():
        prepare()
        for copy in bulk:
            copy.wait()
        source(1, first_part, everywhere, inc_load.wait)

    def second_source():
        source(1 + first_part, rows - 2 - first_part, everywhere)

    for copy in small[:3] + last_row + first_row + col_loads[:2]:
        copy.wait()
    pl.when(early)(first_source)
    peers = 2 + lax.div(gy + ny - 1, ny) + lax.div(2 * ny - 2 - gy, ny)
    pl.semaphore_wait(barrier, peers)
    for side in ("south", "north"):
        start(stat_copies, side)
        start(one, side)
    for side in ("east", "west"):
        start(stat_copies, side)
        start(one, side)
    pl.when(late)(first_source)
    second_source()
    for copy in col_loads[2:] + ci_loads:
        copy.wait()
    for side in sides:
        wait_recv(stat_copies, side)
    prepare_edges()
    for side in sides:
        wait_recv(one, side)
    edge_columns((1,))
    start(two, "north")
    edge_columns((0,))
    start(two, "south")
    odd = lax.rem(gx, 2)
    for near in (0, 1):
        source((odd if near == 0 else 1 - odd) * (rows - 1), 1, everywhere)
        for turn, side, i in ((near, "west", 0), (1 - near, "east", rows - 1)):

            @pl.when(odd == turn)
            def _(side=side, i=i):
                insert_columns((i,))
                start(two, side)

    insert_columns(range(1, rows - 1))
    looped(1, rows - 1, lambda i: transport([(i, jt) for jt in everywhere]))
    transport([(0, jt) for jt in everywhere], skip_w=True)
    transport([(rows - 1, jt) for jt in everywhere], skip_e=True)
    for side in ("west", "east"):
        wait_recv(two, side)
    finish_row(rows - 1)
    finish_row(0)
    wait_recv(two, "south")
    finish_column(1)
    wait_recv(two, "north")
    finish_column(0)
    for group in (stat_copies, one, two):
        for side in sides:
            wait_send(group, side)


def body(
    spectrum,
    adjoint_in,
    current_x,
    current_y,
    wind_x,
    wind_y,
    land_mask,
    ice_mask,
    group_speed,
    growth_rate,
    dissipation,
):
    rows, cols, bins = spectrum.shape
    freqs = group_speed.shape[0]
    wave = np.zeros((8, -(-bins // LANES) * LANES), np.float32)
    wave[0, :bins], wave[1, :bins] = directions(bins)
    mains = bins // LANES
    tail = bins - mains * LANES
    tall = cols + 2 * PAD
    f32 = jnp.float32
    any_space = pl.BlockSpec(memory_space=pl.ANY)
    return pl.pallas_call(
        kernel,
        out_shape=pltpu.VMEM((rows, cols, bins), f32),
        in_specs=[any_space] * 12,
        out_specs=pl.BlockSpec(memory_space=pltpu.VMEM),
        scratch_shapes=[
            pltpu.VMEM((rows + 2, mains, tall, LANES), f32),
            pltpu.VMEM((rows + 2, tall, tail), f32),
            pltpu.VMEM((rows + 2, mains, tall, LANES), f32),
            pltpu.VMEM((rows + 2, tall, tail), f32),
            pltpu.VMEM((rows, cols, bins), f32),
            pltpu.VMEM((rows, cols // 8, mains + 1, 8, LANES), f32),
            pltpu.VMEM((rows + 1, cols, LANES), f32),
            pltpu.VMEM((rows + 1, cols, LANES), f32),
            pltpu.VMEM((rows, tall, LANES), f32),
            pltpu.VMEM((rows, tall, LANES), f32),
            pltpu.VMEM((rows, cols, LANES), f32),
            pltpu.VMEM((rows, cols, LANES), f32),
            pltpu.VMEM((rows, cols, LANES), f32),
            pltpu.VMEM((cols // 8, mains + 1, 8, LANES), f32),
            pltpu.VMEM((rows, cols // 8, 8, LANES), f32),
            pltpu.VMEM((rows, cols // 8, 8, LANES), f32),
            pltpu.VMEM((6, rows, bins), f32),
            pltpu.VMEM((2, rows, bins), f32),
            pltpu.VMEM((4, rows, bins), f32),
            pltpu.VMEM((2, 11, rows, LANES), f32),
            pltpu.VMEM((3, 1, freqs), f32),
            pltpu.VMEM(wave.shape, f32),
            pltpu.VMEM((8, LANES), f32),
            pltpu.VMEM((5 * (mains + 1), 8, LANES), f32),
            pltpu.VMEM((4, rows, cols), f32),
            pltpu.VMEM((2, rows, cols), jnp.int32),
            pltpu.VMEM((4, rows, cols), f32),
            pltpu.VMEM((4, rows, cols), jnp.int32),
            pltpu.VMEM((32, LANES), f32),
            pltpu.SemaphoreType.DMA((3 * (mains + 1) + 17,)),
            pltpu.SemaphoreType.DMA((24,)),
            pltpu.SemaphoreType.DMA((24,)),
        ],
        compiler_params=pltpu.CompilerParams(
            collective_id=0, has_side_effects=True, vmem_limit_bytes=50 * 1024 * 1024
        ),
    )(
        spectrum,
        adjoint_in,
        current_x,
        current_y,
        wind_x,
        wind_y,
        land_mask,
        ice_mask,
        group_speed.reshape(1, freqs),
        growth_rate.reshape(1, freqs),
        dissipation.reshape(1, freqs),
        jnp.asarray(wave),
    )


def solution(mesh):
    cells = P("gx", "gy", None)
    placed = (cells, cells) + (P("gx", "gy"),) * 6 + (P(),) * 3
    return jax.shard_map(body, mesh=mesh, in_specs=placed, out_specs=cells, check_vma=False)
```

```python
import math

import jax
import jax.numpy as jnp
import numpy as np
from jax import lax
from jax.experimental import pallas as pl
from jax.experimental.pallas import tpu as pltpu
from jax.sharding import PartitionSpec as P

DIRS = 36
LANES = 128
LEAST_SPEED = 0.1
MOST_CURRENT = 0.08
PAD = 8
MESH = pl.DeviceIdType.MESH


def directions(bins):
    angles = np.float32(2.0 * math.pi / DIRS) * (np.arange(DIRS, dtype=np.float32) + np.float32(0.5))
    per_dir = bins // DIRS
    return np.repeat(np.cos(angles), per_dir), np.repeat(np.sin(angles), per_dir)


def one_way(heading):
    sure = 1.001 * MOST_CURRENT / LEAST_SPEED
    starts = range(0, heading.size, LANES)
    forward = [t for t, b in enumerate(starts) if np.all(heading[b : b + LANES] > sure)]
    backward = [t for t, b in enumerate(starts) if np.all(heading[b : b + LANES] < -sure)]
    return forward, backward


def kernel(
    spec_hbm,
    adj_hbm,
    cx_hbm,
    cy_hbm,
    wx_hbm,
    wy_hbm,
    land_hbm,
    ice_hbm,
    speed_hbm,
    growth_hbm,
    loss_hbm,
    wave_hbm,
    out,
    sp_main,
    sp_tail,
    ss_main,
    ss_tail,
    inc,
    adv,
    oxs,
    pxs,
    oys,
    pys,
    wxs,
    wys,
    seas,
    fx,
    part,
    level,
    col,
    ci,
    sc,
    dc,
    par_in,
    wave,
    par,
    tab,
    stat_f,
    stat_i,
    nb_f,
    nb_i,
    ext,
    load_sem,
    send_sem,
    recv_sem,
):
    rows, cols, bins = spec_hbm.shape
    mains = bins // LANES
    tail = bins - mains * LANES
    tiles = cols // 8
    pieces = mains + 1
    gx = lax.axis_index("gx")
    gy = lax.axis_index("gy")
    nx = lax.axis_size("gx")
    ny = lax.axis_size("gy")
    east = lax.rem(gx + 1, nx)
    west = lax.rem(gx + nx - 1, nx)
    has_north = gy < ny - 1
    has_south = gy > 0
    body = pl.ds(PAD, cols)

    barrier = pltpu.get_barrier_semaphore()
    for target in (east, west):
        pl.semaphore_signal(barrier, inc=1, device_id={"gx": target}, device_id_type=MESH)

    @pl.when(has_north)
    def _():
        pl.semaphore_signal(barrier, inc=1, device_id={"gy": gy + 1}, device_id_type=MESH)

    @pl.when(has_south)
    def _():
        pl.semaphore_signal(barrier, inc=1, device_id={"gy": gy - 1}, device_id_type=MESH)

    def local(src, dst, k):
        return pltpu.make_async_copy(src, dst, load_sem.at[k])

    def loads_of(low, count, base):
        copies = []
        for t in range(pieces):
            src_lanes = pl.ds(t * LANES, LANES if t < mains else tail)
            src = spec_hbm.at[pl.ds(low, count), :, src_lanes]
            if t < mains:
                dst = sp_main.at[pl.ds(low + 1, count), t, body, :]
            else:
                dst = sp_tail.at[pl.ds(low + 1, count), body, :]
            copies.append(local(src, dst, base + t))
        return copies

    first_row = loads_of(0, 1, 0)
    last_row = loads_of(rows - 1, 1, pieces)
    bulk = loads_of(1, rows - 2, 2 * pieces)
    base = 3 * pieces
    small = [
        local(land_hbm, stat_i.at[0], base),
        local(cx_hbm, stat_f.at[0], base + 1),
        local(cy_hbm, stat_f.at[1], base + 2),
        local(wx_hbm, stat_f.at[2], base + 3),
        local(wy_hbm, stat_f.at[3], base + 4),
        local(ice_hbm, stat_i.at[1], base + 5),
        local(speed_hbm, par_in.at[0], base + 6),
        local(growth_hbm, par_in.at[1], base + 7),
        local(loss_hbm, par_in.at[2], base + 8),
        local(wave_hbm, wave, base + 9),
    ]
    inc_load = local(adj_hbm, inc, base + 10)
    col_loads = [
        local(spec_hbm.at[:, j, :], col.at[k], base + 10 + k)
        for k, j in ((1, 0), (4, cols - 1), (2, 1), (3, cols - 2))
    ]
    ci_loads = [
        local(adj_hbm.at[:, j, :], ci.at[k], base + 15 + k) for k, j in ((0, 0), (1, cols - 1))
    ]
    for copy in small + last_row + first_row + col_loads + bulk + ci_loads + [inc_load]:
        copy.start()

    def remote(src, dst, k, device):
        return pltpu.make_async_remote_copy(
            src_ref=src,
            dst_ref=dst,
            send_sem=send_sem.at[k],
            recv_sem=recv_sem.at[k],
            device_id=device,
            device_id_type=MESH,
        )

    to_east, to_west = {"gx": east}, {"gx": west}
    to_north, to_south = {"gy": gy + 1}, {"gy": gy - 1}

    used = iter(range(24))

    def runs(skip):
        spans, low = [], 0
        for t in sorted(skip) + [pieces]:
            if t > low:
                spans.append((low, t))
            low = t + 1
        return spans

    def edge(main, last, lines, side, skip):
        copies = []
        for low, high in runs(skip):
            if side in ("north", "south"):
                lanes = pl.ds(low * LANES, min(high * LANES, bins) - low * LANES)
                top = lines.shape[0] - 1
                src, dst, device = (top - 1, 0, to_north) if side == "north" else (1, top, to_south)
                copies.append(
                    remote(lines.at[src, :, lanes], lines.at[dst, :, lanes], next(used), device)
                )
                continue
            src, dst, device = (rows, 0, to_east) if side == "east" else (1, rows + 1, to_west)
            whole = pl.ds(low, min(high, mains) - low)
            copies.append(
                remote(main.at[src, whole, body, :], main.at[dst, whole, body, :], next(used), device)
            )
            if high == pieces:
                copies.append(
                    remote(last.at[src, body, :], last.at[dst, body, :], next(used), device)
                )
        return copies

    sides = ("east", "west", "north", "south")
    stat_copies = {}
    for s, (side, device, field) in enumerate(
        (("east", to_east, 0), ("west", to_west, 0), ("north", to_north, 1), ("south", to_south, 1))
    ):
        stat_copies[side] = [
            remote(stat_i.at[0], nb_i.at[s], next(used), device),
            remote(stat_f.at[field], nb_f.at[s], next(used), device),
        ]
    cosine, sine = directions(bins)
    (eastward, westward), (northward, southward) = one_way(cosine), one_way(sine)
    idle_one = {"east": westward, "west": eastward, "north": southward, "south": northward}
    idle_two = {"east": eastward, "west": westward, "north": northward, "south": southward}
    one = {side: edge(sp_main, sp_tail, col, side, idle_one[side]) for side in sides}
    two = {side: edge(ss_main, ss_tail, sc, side, idle_two[side]) for side in sides}

    sends_ok = {"east": None, "west": None, "north": has_north, "south": has_south}
    recvs_ok = {"east": None, "west": None, "north": has_south, "south": has_north}

    def guarded(condition, run):
        if condition is None:
            run()
        else:
            pl.when(condition)(run)

    def start(group, side):
        guarded(sends_ok[side], lambda: [copy.start() for copy in group[side]] and None)

    def wait_recv(group, side):
        guarded(recvs_ok[side], lambda: [copy.wait_recv() for copy in group[side]] and None)

    def wait_send(group, side):
        guarded(sends_ok[side], lambda: [copy.wait_send() for copy in group[side]] and None)

    lane = lax.broadcasted_iota(jnp.int32, (32, LANES), 1)
    row = lax.broadcasted_iota(jnp.int32, (32, LANES), 0)

    def widened(values):
        ext[...] = jnp.zeros((32, LANES), jnp.float32)
        ext[pl.ds(0, rows), pl.ds(0, cols)] = values
        return ext[...]

    def sea_of(mask):
        return (1 - mask).astype(jnp.float32)

    def around_lon(mine, from_east, from_west):
        up = pltpu.roll(widened(from_east), rows, 0)
        down = pltpu.roll(widened(from_west), 8, 0)
        return jnp.where(row == rows, up, jnp.where(row == 31, down, mine))

    def around_lat(mine, from_north, from_south):
        up = pltpu.roll(widened(from_north), cols, 1)
        down = pltpu.roll(widened(from_south), LANES - cols, 1)
        up = jnp.where(has_north, up, 0.0)
        down = jnp.where(has_south, down, 0.0)
        return jnp.where(lane == cols, up, jnp.where(lane == LANES - 1, down, mine))

    def spread(places):
        turned = {}
        for field, dst, spot, column, r in places:
            if id(field) not in turned:
                turned[id(field)] = jnp.transpose(field)
        for field, dst, spot, column, r in sorted(places, key=lambda place: place[4]):
            count = column.stop - column.start
            dst[spot] = jnp.broadcast_to(turned[id(field)][column, r : r + 1], (count, LANES))

    inside = slice(0, cols)
    inside_at = pl.ds(PAD, cols)

    def lon_faces(sea_lon, drift_lon):
        opened = sea_lon * pltpu.roll(sea_lon, 31, 0)
        return opened, opened * (0.5 * (drift_lon + pltpu.roll(drift_lon, 31, 0)))

    def lat_faces(sea_lat, drift_lat):
        opened = sea_lat * pltpu.roll(sea_lat, LANES - 1, 1)
        return opened, opened * (0.5 * (drift_lat + pltpu.roll(drift_lat, LANES - 1, 1)))

    def prepare():
        for copy in small[3:]:
            copy.wait()
        par[...] = jnp.zeros((8, LANES), jnp.float32)
        freqs = speed_hbm.shape[1]
        for k in range(3):
            par[pl.ds(k, 1), pl.ds(0, freqs)] = par_in[k]
        per_freq = par[...]
        bin_lane = lax.broadcasted_iota(jnp.int32, (8, LANES), 1)
        for t in range(pieces):
            freq = lax.rem(bin_lane + t * LANES, freqs)
            picked = jnp.take_along_axis(per_freq, freq, axis=1)
            full = (8, LANES)
            speed = jnp.broadcast_to(picked[0:1], full)
            growth = jnp.broadcast_to(picked[1:2], full)
            cosine = jnp.broadcast_to(wave[pl.ds(0, 1), pl.ds(t * LANES, LANES)], full)
            sine = jnp.broadcast_to(wave[pl.ds(1, 1), pl.ds(t * LANES, LANES)], full)
            tab[t] = speed * cosine
            tab[pieces + t] = speed * sine
            tab[2 * pieces + t] = growth * cosine
            tab[3 * pieces + t] = growth * sine
            tab[4 * pieces + t] = jnp.broadcast_to(picked[2:3], full)
        sea = widened(sea_of(stat_i[0]))
        wet = widened(sea_of(stat_i[1])) * sea
        every = range(rows)
        lon = lon_faces(sea, widened(stat_f[0]))
        lat = lat_faces(sea, widened(stat_f[1]))
        breeze = [widened(stat_f[2]) * wet, widened(stat_f[3]) * wet]
        places = []
        for r in every:
            places += [(field, dst, r, inside, r) for field, dst in zip(breeze + [sea], (wxs, wys, seas))]
            places += [(field, dst, (r, inside_at), inside, r) for field, dst in zip(lat, (oys, pys))]
            if r < rows - 1:
                places += [(field, dst, r + 1, inside, r) for field, dst in zip(lon, (oxs, pxs))]
        spread(places)
        for dst in (oys, pys):
            for r in every:
                dst[r, pl.ds(0, PAD), :] = jnp.zeros((PAD, LANES), jnp.float32)

    def prepare_edges():
        sea = widened(sea_of(stat_i[0]))
        sea_lon = around_lon(sea, sea_of(nb_i[1]), sea_of(nb_i[0]))
        sea_lat = around_lat(sea, sea_of(nb_i[3]), sea_of(nb_i[2]))
        drift_lon = around_lon(widened(stat_f[0]), nb_f[1], nb_f[0])
        drift_lat = around_lat(widened(stat_f[1]), nb_f[3], nb_f[2])
        wet = widened(sea_of(stat_i[1])) * sea
        lon = lon_faces(sea_lon, drift_lon)
        lat = lat_faces(sea_lat, drift_lat)
        places = []
        for field, dst in zip(lon, (oxs, pxs)):
            places += [(field, dst, 0, inside, 31), (field, dst, rows, inside, rows - 1)]
        spread(places)
        fields = list(lon) + [pltpu.roll(field, 1, 0) for field in lon]
        fields += list(lat) + [pltpu.roll(field, 1, 1) for field in lat]
        fields += [widened(stat_f[2]) * wet, widened(stat_f[3]) * wet, sea]
        for k, j in enumerate((0, cols - 1)):
            for m, field in enumerate(fields):
                dc[k, m] = jnp.broadcast_to(field[0:rows, j : j + 1], (rows, LANES))

    def width_of(t):
        return LANES if t < mains else tail

    def at(main, last, r, t, line):
        if t < mains:
            return main[r, t, pl.ds(line, 8), :]
        return last[r, pl.ds(line, 8), :]

    def put(main, last, r, t, line, value):
        if t < mains:
            main[r, t, pl.ds(line, 8), :] = value
        else:
            last[r, pl.ds(line, 8), :] = value

    def table(k, t):
        return tab[k * pieces + t, :, pl.ds(0, width_of(t))]

    def faces(i, jt, t):
        cut = (slice(None), slice(0, width_of(t)))
        line = PAD + 8 * jt
        cos_speed, sin_speed = table(0, t), table(1, t)
        spot = pl.ds(8 * jt, 8)
        a_e = oxs[i + 1, spot, :][cut] * cos_speed + pxs[i + 1, spot, :][cut]
        a_w = oxs[i, spot, :][cut] * cos_speed + pxs[i, spot, :][cut]
        a_n = oys[i, pl.ds(line, 8), :][cut] * sin_speed + pys[i, pl.ds(line, 8), :][cut]
        a_s = oys[i, pl.ds(line - 1, 8), :][cut] * sin_speed + pys[i, pl.ds(line - 1, 8), :][cut]
        return a_e, a_w, a_n, a_s

    scale = 1.0 / bins

    def lon_flux(i, jt, t, from_west=False):
        cut = (slice(None), slice(0, width_of(t)))
        spot = pl.ds(8 * jt, 8)
        line = PAD + 8 * jt
        pace = oxs[i + 1, spot, :][cut] * table(0, t) + pxs[i + 1, spot, :][cut]
        here, e = at(sp_main, sp_tail, i + 1, t, line), at(sp_main, sp_tail, i + 2, t, line)
        if from_west:
            return jnp.where(pace > 0.0, pace * here, jnp.where(pace < 0.0, pace * e, 0.0))
        return pace * jnp.where(pace < 0.0, e, here)

    def tally(i, jt, parts):
        whole = parts[0]
        for more in parts[1:mains]:
            whole = whole + more
        part[i, jt] = whole
        part[i, jt, :, pl.ds(0, tail)] = whole[:, :tail] + parts[mains]

    def prime(i, jts):
        for jt in jts:
            for t in range(pieces):
                fx[jt, t, :, pl.ds(0, width_of(t))] = lon_flux(i - 1, jt, t, True)

    def advect(i, jts):
        for jt in jts:
            parts = []
            spot = pl.ds(PAD + 8 * jt, 8)
            under = pl.ds(PAD + 8 * jt - 1, 8)
            for t in range(pieces):
                width = width_of(t)
                cut = (slice(None), slice(0, width))
                sin_speed = table(1, t)
                a_n = oys[i, spot, :][cut] * sin_speed + pys[i, spot, :][cut]
                a_s = oys[i, under, :][cut] * sin_speed + pys[i, under, :][cut]
                line = PAD + 8 * jt
                here = at(sp_main, sp_tail, i + 1, t, line)
                n = at(sp_main, sp_tail, i + 1, t, line + 1)
                s = at(sp_main, sp_tail, i + 1, t, line - 1)
                f_w = fx[jt, t, :, pl.ds(0, width)]
                f_e = lon_flux(i, jt, t)
                fx[jt, t, :, pl.ds(0, width)] = f_e
                lat = a_n * jnp.where(a_n < 0.0, n, here) - a_s * jnp.where(a_s > 0.0, s, here)
                moved = here - (f_e - f_w) - lat
                adv[i, jt, t, :, pl.ds(0, width)] = moved
                parts.append(moved)
            tally(i, jt, parts)

    def gather(low, count, jt, tall):
        block = (pl.ds(low, count), pl.ds(jt, tall))
        level[block] = jnp.broadcast_to(
            jnp.sum(part[block], axis=3, keepdims=True) * scale, (count, tall, 8, LANES)
        )

    def weigh(i, jts):
        for jt in jts:
            parts = []
            spot = pl.ds(8 * jt, 8)
            energy = level[i, jt]
            for t in range(pieces):
                width = width_of(t)
                cut = (slice(None), slice(0, width))
                moved = adv[i, jt, t, :, pl.ds(0, width)]
                blow = wxs[i, spot, :][cut] * table(2, t) + wys[i, spot, :][cut] * table(3, t)
                gain = jnp.maximum(blow, 0.0) + seas[i, spot, :][cut]
                loss = table(4, t) * moved
                damp = 1.0 + energy[cut] * loss
                square = damp * damp
                inverse = pl.reciprocal(square, approx=True)
                inverse = inverse * (2.0 - square * inverse)
                weighted = inc[i, spot, pl.ds(t * LANES, width)] * gain * inverse
                put(ss_main, ss_tail, i + 1, t, PAD + 8 * jt, weighted)
                parts.append(weighted * loss * moved)
            tally(i, jt, parts)

    def settle(i, jts):
        for jt in jts:
            line = PAD + 8 * jt
            pull = level[i, jt]
            for t in range(pieces):
                value = at(ss_main, ss_tail, i + 1, t, line) - pull[:, : width_of(t)]
                put(ss_main, ss_tail, i + 1, t, line, value)

    def source(low, count, jts, before_weigh=None):
        jts = list(jts)
        prime(low, jts)
        spans = [(jts[0], len(jts))] if jts[-1] - jts[0] == len(jts) - 1 else [(jt, 1) for jt in jts]
        for step in (advect, weigh, settle):
            if step is weigh and before_weigh is not None:
                before_weigh()
            if count == 1:
                step(low, jts)
            else:
                looped(low, low + count, lambda i: step(i, jts))
            if step is not settle:
                for jt, tall in spans:
                    gather(low, count, jt, tall)

    row_at = lax.broadcasted_iota(jnp.int32, (rows, LANES), 0)

    def line(main, last, r, t, place):
        if t < mains:
            return main.at[r, t, pl.ds(place, 1), :]
        return last.at[r, pl.ds(place, 1), :]

    def lanes_of(t):
        return pl.ds(t * LANES, width_of(t))

    def lane_sum(parts):
        whole = parts[0]
        for more in parts[1:mains]:
            whole = whole + more
        return jnp.sum(whole, axis=1, keepdims=True) + jnp.sum(parts[mains], axis=1, keepdims=True)

    def wide_table(k, t):
        return jnp.broadcast_to(tab[k * pieces + t, pl.ds(0, 1), pl.ds(0, width_of(t))], (rows, width_of(t)))

    def edge_columns(ends):
        places = (PAD, PAD + cols - 1)
        sums = [[], []]
        for k in ends:
            here_at, n_at, s_at = ((1, 2, 0), (4, 5, 3))[k]
            for t in range(pieces):
                width = width_of(t)
                coef = [dc[k, m][:, :width] for m in range(8)]
                cos_speed, sin_speed = wide_table(0, t), wide_table(1, t)
                here = col[here_at, :, lanes_of(t)]
                n, s = col[n_at, :, lanes_of(t)], col[s_at, :, lanes_of(t)]
                e_end = line(sp_main, sp_tail, rows + 1, t, places[k])[...]
                w_end = line(sp_main, sp_tail, 0, t, places[k])[...]
                at_row = row_at[:, :width]
                e = jnp.where(at_row == rows - 1, e_end, pltpu.roll(here, rows - 1, 0))
                w = jnp.where(at_row == 0, w_end, pltpu.roll(here, 1, 0))
                a_e = coef[0] * cos_speed + coef[1]
                a_w = coef[2] * cos_speed + coef[3]
                a_n = coef[4] * sin_speed + coef[5]
                a_s = coef[6] * sin_speed + coef[7]
                lon = a_e * jnp.where(a_e < 0.0, e, here) - a_w * jnp.where(a_w > 0.0, w, here)
                lat = a_n * jnp.where(a_n < 0.0, n, here) - a_s * jnp.where(a_s > 0.0, s, here)
                moved = here - lon - lat
                sc[1 + k, :, lanes_of(t)] = moved
                sums[k].append(moved)
        energies = {k: lane_sum(sums[k]) * scale for k in ends}
        pulls = [[], []]
        for k in ends:
            energy = jnp.broadcast_to(energies[k], (rows, LANES))
            for t in range(pieces):
                width = width_of(t)
                wind_x, wind_y, open_sea = [dc[k, m][:, :width] for m in range(8, 11)]
                moved = sc[1 + k, :, lanes_of(t)]
                blow = wind_x * wide_table(2, t) + wind_y * wide_table(3, t)
                gain = jnp.maximum(blow, 0.0) + open_sea
                loss = wide_table(4, t) * moved
                damp = 1.0 + energy[:, :width] * loss
                square = damp * damp
                inverse = pl.reciprocal(square, approx=True)
                inverse = inverse * (2.0 - square * inverse)
                weighted = ci[k, :, lanes_of(t)] * gain * inverse
                sc[1 + k, :, lanes_of(t)] = weighted
                pulls[k].append(weighted * loss * moved)
        ends_pull = {k: lane_sum(pulls[k]) * scale for k in ends}
        for k in ends:
            pull = jnp.broadcast_to(ends_pull[k], (rows, LANES))
            for t in range(pieces):
                sc[1 + k, :, lanes_of(t)] = sc[1 + k, :, lanes_of(t)] - pull[:, : width_of(t)]

    def insert_columns(which):
        for i in which:
            for k, place in enumerate((PAD, PAD + cols - 1)):
                for t in range(pieces):
                    target = line(ss_main, ss_tail, i + 1, t, place)
                    target[...] = sc[1 + k, pl.ds(i, 1), lanes_of(t)]

    def transport(cells, skip_e=False, skip_w=False):
        for i, jt in cells:
            for t in range(pieces):
                a_e, a_w, a_n, a_s = faces(i, jt, t)
                place = PAD + 8 * jt
                here = at(ss_main, ss_tail, i + 1, t, place)
                n = at(ss_main, ss_tail, i + 1, t, place + 1)
                s = at(ss_main, ss_tail, i + 1, t, place - 1)
                total = here
                if not skip_e:
                    e = at(ss_main, ss_tail, i + 2, t, place)
                    total = total + jnp.maximum(a_e, 0.0) * (e - here)
                if not skip_w:
                    w = at(ss_main, ss_tail, i, t, place)
                    total = total + jnp.minimum(a_w, 0.0) * (here - w)
                if jt == tiles - 1:
                    total = total + jnp.where(a_n > 0.0, a_n * (n - here), 0.0)
                else:
                    total = total + jnp.maximum(a_n, 0.0) * (n - here)
                if jt == 0:
                    total = total + jnp.where(a_s < 0.0, a_s * (here - s), 0.0)
                else:
                    total = total + jnp.minimum(a_s, 0.0) * (here - s)
                out[i, pl.ds(8 * jt, 8), lanes_of(t)] = total

    def finish_row(i):
        for jt in range(tiles):
            spot = pl.ds(8 * jt, 8)
            for t in range(pieces):
                if t in (idle_two["east"] if i == 0 else idle_two["west"]):
                    continue
                cut = (slice(None), slice(0, width_of(t)))
                here = at(ss_main, ss_tail, i + 1, t, PAD + 8 * jt)
                if i == 0:
                    a_w = oxs[0, spot, :][cut] * table(0, t) + pxs[0, spot, :][cut]
                    term = jnp.minimum(a_w, 0.0) * (here - at(ss_main, ss_tail, 0, t, PAD + 8 * jt))
                else:
                    a_e = oxs[rows, spot, :][cut] * table(0, t) + pxs[rows, spot, :][cut]
                    far = at(ss_main, ss_tail, rows + 1, t, PAD + 8 * jt)
                    term = jnp.maximum(a_e, 0.0) * (far - here)
                out[i, spot, lanes_of(t)] = out[i, spot, lanes_of(t)] + term

    def finish_column(k):
        for t in range(pieces):
            width = width_of(t)
            here = sc[1 + k, :, lanes_of(t)]
            if k == 0:
                a_s = dc[0, 6][:, :width] * wide_table(1, t) + dc[0, 7][:, :width]
                term = jnp.where(a_s < 0.0, a_s * (here - sc[0, :, lanes_of(t)]), 0.0)
            else:
                a_n = dc[1, 4][:, :width] * wide_table(1, t) + dc[1, 5][:, :width]
                term = jnp.where(a_n > 0.0, a_n * (sc[3, :, lanes_of(t)] - here), 0.0)
            ci[k, :, lanes_of(t)] = term
        place = pl.ds(0 if k == 0 else cols - 1, 1)
        for i in range(rows):
            for t in range(pieces):
                term = ci[k, pl.ds(i, 1), lanes_of(t)]
                out[i, place, lanes_of(t)] = out[i, place, lanes_of(t)] + term

    def looped(low, high, run):
        def step(i, carry):
            run(i)
            return carry

        lax.fori_loop(low, high, step, 0)

    everywhere = range(tiles)
    early = gy == ny // 2
    late = gy != ny // 2
    first_part = (rows - 2) * 3 // 11

    def first_source():
        prepare()
        for copy in bulk:
            copy.wait()
        source(1, first_part, everywhere, inc_load.wait)

    def second_source():
        source(1 + first_part, rows - 2 - first_part, everywhere)

    for copy in small[:3] + last_row + first_row + col_loads[:2]:
        copy.wait()
    pl.when(early)(first_source)
    peers = 2 + lax.div(gy + ny - 1, ny) + lax.div(2 * ny - 2 - gy, ny)
    pl.semaphore_wait(barrier, peers)
    for side in ("south", "north"):
        start(stat_copies, side)
        start(one, side)
    for side in ("east", "west"):
        start(stat_copies, side)
        start(one, side)
    pl.when(late)(first_source)
    second_source()
    for copy in col_loads[2:] + ci_loads:
        copy.wait()
    for side in sides:
        wait_recv(stat_copies, side)
    prepare_edges()
    for side in sides:
        wait_recv(one, side)
    edge_columns((1,))
    start(two, "north")
    edge_columns((0,))
    start(two, "south")
    odd = lax.rem(gx, 2)
    for near in (0, 1):
        source((odd if near == 0 else 1 - odd) * (rows - 1), 1, everywhere)
        for turn, side, i in ((near, "west", 0), (1 - near, "east", rows - 1)):

            @pl.when(odd == turn)
            def _(side=side, i=i):
                insert_columns((i,))
                start(two, side)

    insert_columns(range(1, rows - 1))
    looped(1, rows - 1, lambda i: transport([(i, jt) for jt in everywhere]))
    transport([(0, jt) for jt in everywhere], skip_w=True)
    transport([(rows - 1, jt) for jt in everywhere], skip_e=True)
    for side in ("west", "east"):
        wait_recv(two, side)
    finish_row(rows - 1)
    finish_row(0)
    wait_recv(two, "south")
    finish_column(1)
    wait_recv(two, "north")
    finish_column(0)
    for group in (stat_copies, one, two):
        for side in sides:
            wait_send(group, side)


def body(
    spectrum,
    adjoint_in,
    current_x,
    current_y,
    wind_x,
    wind_y,
    land_mask,
    ice_mask,
    group_speed,
    growth_rate,
    dissipation,
):
    rows, cols, bins = spectrum.shape
    freqs = group_speed.shape[0]
    wave = np.zeros((8, -(-bins // LANES) * LANES), np.float32)
    wave[0, :bins], wave[1, :bins] = directions(bins)
    mains = bins // LANES
    tail = bins - mains * LANES
    tall = cols + 2 * PAD
    f32 = jnp.float32
    any_space = pl.BlockSpec(memory_space=pl.ANY)
    return pl.pallas_call(
        kernel,
        out_shape=pltpu.VMEM((rows, cols, bins), f32),
        in_specs=[any_space] * 12,
        out_specs=pl.BlockSpec(memory_space=pltpu.VMEM),
        scratch_shapes=[
            pltpu.VMEM((rows + 2, mains, tall, LANES), f32),
            pltpu.VMEM((rows + 2, tall, tail), f32),
            pltpu.VMEM((rows + 2, mains, tall, LANES), f32),
            pltpu.VMEM((rows + 2, tall, tail), f32),
            pltpu.VMEM((rows, cols, bins), f32),
            pltpu.VMEM((rows, cols // 8, mains + 1, 8, LANES), f32),
            pltpu.VMEM((rows + 1, cols, LANES), f32),
            pltpu.VMEM((rows + 1, cols, LANES), f32),
            pltpu.VMEM((rows, tall, LANES), f32),
            pltpu.VMEM((rows, tall, LANES), f32),
            pltpu.VMEM((rows, cols, LANES), f32),
            pltpu.VMEM((rows, cols, LANES), f32),
            pltpu.VMEM((rows, cols, LANES), f32),
            pltpu.VMEM((cols // 8, mains + 1, 8, LANES), f32),
            pltpu.VMEM((rows, cols // 8, 8, LANES), f32),
            pltpu.VMEM((rows, cols // 8, 8, LANES), f32),
            pltpu.VMEM((6, rows, bins), f32),
            pltpu.VMEM((2, rows, bins), f32),
            pltpu.VMEM((4, rows, bins), f32),
            pltpu.VMEM((2, 11, rows, LANES), f32),
            pltpu.VMEM((3, 1, freqs), f32),
            pltpu.VMEM(wave.shape, f32),
            pltpu.VMEM((8, LANES), f32),
            pltpu.VMEM((5 * (mains + 1), 8, LANES), f32),
            pltpu.VMEM((4, rows, cols), f32),
            pltpu.VMEM((2, rows, cols), jnp.int32),
            pltpu.VMEM((4, rows, cols), f32),
            pltpu.VMEM((4, rows, cols), jnp.int32),
            pltpu.VMEM((32, LANES), f32),
            pltpu.SemaphoreType.DMA((3 * (mains + 1) + 17,)),
            pltpu.SemaphoreType.DMA((24,)),
            pltpu.SemaphoreType.DMA((24,)),
        ],
        compiler_params=pltpu.CompilerParams(
            collective_id=0, has_side_effects=True, vmem_limit_bytes=50 * 1024 * 1024
        ),
    )(
        spectrum,
        adjoint_in,
        current_x,
        current_y,
        wind_x,
        wind_y,
        land_mask,
        ice_mask,
        group_speed.reshape(1, freqs),
        growth_rate.reshape(1, freqs),
        dissipation.reshape(1, freqs),
        jnp.asarray(wave),
    )


def solution(mesh):
    cells = P("gx", "gy", None)
    placed = (cells, cells) + (P("gx", "gy"),) * 6 + (P(),) * 3
    return jax.shard_map(body, mesh=mesh, in_specs=placed, out_specs=cells, check_vma=False)
```
